256 devices in a mesh: group: 4 (over y), dp: 8 (over z_lo, core), mp: 8 (over z_hi, x).
Axes of the slice: x: 4, y: 4, z: 8 (z_hi: 2, z_lo: 4; z = z_hi * 4 + z_lo), core: 2. Of those that a mesh axis runs over, the one named last changes fastest.
Arguments:
- patches: bfloat16 [1024, 12800], P(('group', 'mp'), 'dp'), may hold values from -6 to 6
- norm_gain: float32 [12800], P('dp'), may hold values from 0.25 to 1.75
- norm_bias: float32 [12800], P('dp'), may hold values from -3 to 3
- proj_in: bfloat16 [12800, 4096], P('dp', ('group', 'mp')), may hold values from -0.0546875 to 0.0546875
- proj_in_bias: float32 [4096], P(('group', 'mp')), may hold values from -3 to 3
- proj_out: bfloat16 [4096, 4096], P(('group', 'mp'), 'dp'), may hold values from -0.09375 to 0.09375
- proj_out_bias: float32 [4096], P('dp'), may hold values from -3 to 3
- text_rows: bfloat16 [1024, 4096], P(('group', 'mp'), 'dp'), may hold values from -6 to 6
- out_grads: bfloat16 [1024, 4096], P(('group', 'mp'), 'dp'), may hold values from -6 to 6
- gate_weight: bfloat16 [4096, 14336], P('dp', 'mp'), may hold values from -0.09375 to 0.09375
- up_weight: bfloat16 [4096, 14336], P('dp', 'mp'), may hold values from -0.09375 to 0.09375
- down_weight: bfloat16 [14336, 4096], P('mp', 'dp'), may hold values from -0.046875 to 0.046875
- image_counts: int32 [16], replicated, may hold values from 16 to 64, as said below
- image_sequence: int32 [16], replicated, may hold values from 0 to 7, as said below
- image_offsets: int32 [16], replicated, may hold values from 0 to 112, as said below
Outputs:
- projected: bfloat16 [1024, 4096], P(('group', 'mp'), 'dp')
- sequence_grads: bfloat16 [1024, 4096], P(('group', 'mp'), 'dp')
- row_grads: bfloat16 [1024, 4096], P(('group', 'mp'), 'dp')
The draws below stay inside these ranges and needn't reach their ends.
Inputs may be any that keep to these rules, and one draw needn't show every extreme that they name: `image_counts`: image rows lie end to end from row 0 in image order; rows after the last image belong to no image. `image_sequence`: every sequence holds exactly two images. `image_offsets`: the two images of a sequence do not intersect and lie within its 128 rows.
All inputs are finite; a program needn't handle non-finite values.
Results may differ from the reference program's by a relative error of at most 0.0075.
Values may be sent and summed in bfloat16 or wider, within the bound.
No kernel may reach another device: no remote copies, remote signals or barrier semaphores. Data moves between devices by JAX's collectives and lax.ppermute only.
A program may use at most 64 MiB of HBM per device.

```python
import jax
import jax.numpy as jnp
from jax import lax

FEAT = 12800
PROJ = 4096
D = 4096
FF = 14336
TOK_DEV = 128
IMAGES = 16
TOKENS = 1024


def image_plan(key):
    key = jax.random.fold_in(key, 11)
    first_key, order_key, gap_key, second_gap_key = jax.random.split(key, 4)
    counts = jax.random.randint(first_key, (IMAGES,), TOK_DEV // 8, TOK_DEV // 2 + 1).astype(jnp.int32)
    order = jax.random.permutation(order_key, IMAGES).astype(jnp.int32)
    counts = counts.at[order[1]].set(TOK_DEV // 8)
    counts = counts.at[order[2]].set(TOK_DEV // 2)
    slots = jnp.argsort(order, stable=True).astype(jnp.int32)
    sequence = (slots // 2).astype(jnp.int32)
    leading = order[0::2]
    trailing = order[1::2]
    lead_count = counts[leading]
    trail_count = counts[trailing]
    slack = TOK_DEV - lead_count - trail_count
    gap_one = jax.random.randint(gap_key, (IMAGES // 2,), 0, slack + 1).astype(jnp.int32)
    gap_one = gap_one.at[0].set(0)
    gap_two = jax.random.randint(second_gap_key, (IMAGES // 2,), 0, slack - gap_one + 1).astype(jnp.int32)
    gap_two = gap_two.at[0].set(slack[0])
    offsets = jnp.zeros((IMAGES,), jnp.int32)
    offsets = offsets.at[leading].set(gap_one)
    offsets = offsets.at[trailing].set(gap_one + lead_count + gap_two)
    return (counts, sequence, offsets)


def draw_image_counts(key, part):
    return image_plan(key)[0]


def draw_image_sequence(key, part):
    return image_plan(key)[1]


def draw_image_offsets(key, part):
    return image_plan(key)[2]


def levels(rng, extent, cuts, low, top_value):
    def one(position, shards_of):
        heights = jax.random.uniform(jax.random.fold_in(jax.random.fold_in(rng, 6), position), (shards_of,), jnp.float32, low / len(cuts), top_value / len(cuts))
        return jnp.repeat(jnp.exp(heights), extent[position] // shards_of).reshape((-1,) + (1,) * (len(extent) - position - 1))

    gain = one(*cuts[0])
    for cut in cuts[1:]:
        gain = gain * one(*cut)
    return gain


def scatter_about(stream_key, extent, scale, reach, cuts=(), kind=jnp.bfloat16):
    level = levels(stream_key, extent, cuts, -0.22, 0.18) if cuts else 1.0
    array = jax.random.normal(stream_key, extent, jnp.float32) * scale * level
    return jnp.minimum(jnp.maximum(array, -reach), reach).astype(kind)


def setup_inputs(seed: int = 0) -> dict:
    seeds = jax.random.split(jax.random.key(seed), 16)
    return {
        "patches": scatter_about(seeds[0], (TOKENS, FEAT), 1.0, 6.0, ((0, 32), (1, 8))),
        "norm_gain": jnp.clip(1.0 + 0.15 * jax.random.normal(seeds[1], (FEAT,), jnp.float32), 0.25, 1.75),
        "norm_bias": scatter_about(seeds[2], (FEAT,), 0.5, 3.0, ((0, 8),), jnp.float32),
        "proj_in": scatter_about(seeds[3], (FEAT, PROJ), FEAT ** -0.5, 0.0546875, ((0, 8), (1, 32))),
        "proj_in_bias": scatter_about(seeds[4], (PROJ,), 0.5, 3.0, ((0, 32),), jnp.float32),
        "proj_out": scatter_about(seeds[5], (PROJ, D), PROJ ** -0.5, 0.09375, ((0, 32), (1, 8))),
        "proj_out_bias": scatter_about(seeds[6], (D,), 0.5, 3.0, ((0, 8),), jnp.float32),
        "text_rows": scatter_about(seeds[7], (TOKENS, D), 1.0, 6.0, ((0, 32), (1, 8))),
        "out_grads": scatter_about(seeds[8], (TOKENS, D), 1.0, 6.0, ((0, 32), (1, 8))),
        "gate_weight": scatter_about(seeds[9], (D, FF), D ** -0.5, 0.09375, ((0, 8), (1, 8))),
        "up_weight": scatter_about(seeds[10], (D, FF), D ** -0.5, 0.09375, ((0, 8), (1, 8))),
        "down_weight": scatter_about(seeds[11], (FF, D), FF ** -0.5, 0.046875, ((0, 8), (1, 8))),
        "image_counts": draw_image_counts(jax.random.fold_in(seeds[15], 71), 0),
        "image_sequence": draw_image_sequence(jax.random.fold_in(seeds[15], 71), 0),
        "image_offsets": draw_image_offsets(jax.random.fold_in(seeds[15], 71), 0),
    }


def seq_sources(counts, sequence, offsets, length, first, count):
    starts = jnp.cumsum(counts) - counts
    rows = first + jnp.arange(count, dtype=jnp.int32)
    seq = rows // length
    pos = rows % length
    hit = (sequence[None, :] == seq[:, None]) & (offsets[None, :] <= pos[:, None]) & (pos[:, None] < (offsets + counts)[None, :])
    source = lax.optimization_barrier(jnp.sum(jnp.where(hit, starts[None, :] + pos[:, None] - offsets[None, :], 0), axis=1)).astype(jnp.int32)
    return (source, jnp.any(hit, axis=1))

def image_targets(counts, sequence, offsets, length, first, count):
    starts = jnp.cumsum(counts) - counts
    rows = first + jnp.arange(count, dtype=jnp.int32)
    hit = (starts[None, :] <= rows[:, None]) & (rows[:, None] < (starts + counts)[None, :])
    target = lax.optimization_barrier(jnp.sum(jnp.where(hit, sequence[None, :] * length + offsets[None, :] + rows[:, None] - starts[None, :], 0), axis=1)).astype(jnp.int32)
    return (target, jnp.any(hit, axis=1))

def reference(patches, norm_gain, norm_bias, proj_in, proj_in_bias, proj_out, proj_out_bias, text_rows, out_grads, gate_weight, up_weight, down_weight, image_counts, image_sequence, image_offsets):
    values = patches.astype(jnp.float32)
    mean = lax.optimization_barrier(jnp.mean(values, axis=1, keepdims=True))
    centred = values - mean
    spread = lax.optimization_barrier(jnp.mean(centred * centred, axis=1, keepdims=True))
    normed = (centred * jax.lax.rsqrt(spread + 1e-05) * norm_gain + norm_bias).astype(jnp.bfloat16)
    first = jnp.dot(normed, proj_in, preferred_element_type=jnp.float32) + proj_in_bias
    activated = jax.nn.gelu(first, approximate=False).astype(jnp.bfloat16)
    projected = (jnp.dot(activated, proj_out, preferred_element_type=jnp.float32) + proj_out_bias).astype(jnp.bfloat16)
    total = projected.shape[0]
    source, covered = seq_sources(image_counts, image_sequence, image_offsets, TOK_DEV, 0, total)
    inputs = jnp.where(covered[:, None], jnp.take(projected, source, axis=0), text_rows)
    gate = jnp.dot(inputs, gate_weight, preferred_element_type=jnp.float32)
    up = jnp.dot(inputs, up_weight, preferred_element_type=jnp.float32)
    hidden_grad = jnp.dot(out_grads, down_weight.T, preferred_element_type=jnp.float32)
    sig = jax.nn.sigmoid(gate)
    gate_grad = (hidden_grad * up * sig * (1.0 + gate * (1.0 - sig))).astype(jnp.bfloat16)
    up_grad = (hidden_grad * gate * sig).astype(jnp.bfloat16)
    input_grad = jnp.dot(gate_grad, gate_weight.T, preferred_element_type=jnp.float32) + jnp.dot(up_grad, up_weight.T, preferred_element_type=jnp.float32)
    sequence_grads = input_grad.astype(jnp.bfloat16)
    target, valid = image_targets(image_counts, image_sequence, image_offsets, TOK_DEV, 0, total)
    row_grads = jnp.where(valid[:, None], jnp.take(sequence_grads, target, axis=0), jnp.zeros((), jnp.bfloat16)).astype(jnp.bfloat16)
    return (projected, sequence_grads, row_grads)
```

```python
import jax
import jax.numpy as jnp
from jax import lax
from jax.sharding import Mesh
from jax.sharding import PartitionSpec as P

FEAT = 12800
TOK_DEV = 128
ROWS = ("g", "zh", "x")
DP = ("zl", "c")
MP = ("zh", "x")
BF = jnp.bfloat16
F32 = jnp.float32


def from_next(value, axis, k):
    n = lax.axis_size(axis)
    return lax.ppermute(value, axis, [((i + k) % n, i) for i in range(n)])


def swap(value, axis):
    return lax.ppermute(value, axis, [(0, 1), (1, 0)])


def copy_for_each(shard, axis):
    count = lax.axis_size(axis)
    return lax.all_to_all(
        jnp.broadcast_to(shard[None], (count, *shard.shape)), axis, 0, 0, tiled=True
    )


def in_order(own, other, index, dim=0):
    return jnp.where(
        index == 0,
        jnp.concatenate([own, other], axis=dim),
        jnp.concatenate([other, own], axis=dim),
    )


def mm(a, b):
    return jnp.dot(a, b, preferred_element_type=F32)


def mm_t(a, b):
    return lax.dot_general(a, b, (((1,), (1,)), ((), ())), preferred_element_type=F32)


def pick(onehot, rows):
    return mm(onehot, rows).astype(BF)


def three_parts(v):
    hi = lax.reduce_precision(v, 8, 7)
    mid = lax.reduce_precision(v - hi, 8, 7)
    low = v - hi - mid
    return jnp.stack([hi, mid, low]).astype(BF)


def seq_sources(counts, sequence, offsets, rows):
    starts = jnp.cumsum(counts) - counts
    seq = rows // TOK_DEV
    pos = rows % TOK_DEV
    hit = (
        (sequence[None, :] == seq[:, None])
        & (offsets[None, :] <= pos[:, None])
        & (pos[:, None] < (offsets + counts)[None, :])
    )
    source = jnp.sum(jnp.where(hit, starts[None, :] + pos[:, None] - offsets[None, :], 0), axis=1)
    return (source, jnp.any(hit, axis=1))


def image_targets(counts, sequence, offsets, rows):
    starts = jnp.cumsum(counts) - counts
    hit = (starts[None, :] <= rows[:, None]) & (rows[:, None] < (starts + counts)[None, :])
    target = jnp.sum(
        jnp.where(
            hit, sequence[None, :] * TOK_DEV + offsets[None, :] + rows[:, None] - starts[None, :], 0
        ),
        axis=1,
    )
    return (target, jnp.any(hit, axis=1))


def unit_grads(gate, up, hidden_grad):
    sig = jax.nn.sigmoid(gate)
    gate_grad = (hidden_grad * up * sig * (1.0 + gate * (1.0 - sig))).astype(BF)
    up_grad = (hidden_grad * gate * sig).astype(BF)
    return (gate_grad, up_grad)


def local(
    patches,
    norm_gain,
    norm_bias,
    proj_in,
    proj_in_bias,
    proj_out,
    proj_out_bias,
    text_rows,
    out_grads,
    gate_weight,
    up_weight,
    down_weight,
    image_counts,
    image_sequence,
    image_offsets,
):
    g, zl, c, zh, x = (lax.axis_index(a) for a in ("g", "zl", "c", "zh", "x"))
    units = proj_in.shape[1]
    width = gate_weight.shape[1]
    cols = text_rows.shape[1]
    feats = patches.shape[1]

    packed = jnp.concatenate(
        [proj_out, jnp.pad(three_parts(proj_in_bias), ((0, 13), (0, cols - units)))], axis=0
    )
    w_in = [proj_in] + [from_next(proj_in, "g", k) for k in (1, 2, 3)]
    w_out = [packed] + [from_next(packed, "g", k) for k in (1, 2, 3)]

    values = patches.astype(F32)
    sums = jnp.stack([jnp.sum(values, axis=1), jnp.sum(values * values, axis=1)])
    totals = jnp.sum(copy_for_each(sums, DP), axis=0)
    mean = totals[0] / FEAT
    spread = totals[1] / FEAT - mean * mean
    centred = values - mean[:, None]
    normed = (centred * lax.rsqrt(spread + 1e-05)[:, None] * norm_gain + norm_bias).astype(BF)

    mine = jnp.concatenate([text_rows, out_grads, normed], axis=1)
    pair = in_order(mine, swap(mine, "zh"), zh)
    rows = copy_for_each(pair, "x").reshape(-1, 2 * cols + feats)
    text, cotangent, normed_all = rows[:, :cols], rows[:, cols : 2 * cols], rows[:, 2 * cols :]
    count = rows.shape[0]

    first = jnp.concatenate([mm(normed_all, w) for w in w_in], axis=1)
    half = 2 * units
    keep = jnp.where(c == 0, first[:, :half], first[:, half:])
    send = jnp.where(c == 0, first[:, half:], first[:, :half]).astype(BF)
    both = (keep + swap(send, "c").astype(F32)).astype(BF)
    parts = lax.all_to_all(both.reshape(4, count // 4, half), "zl", 0, 0, tiled=True)
    bias = jnp.concatenate([jnp.sum(w[units : units + 3, :units].astype(F32), axis=0) for w in w_out])
    bias = jnp.where(c == 0, bias[:half], bias[half:])
    total = jnp.sum(parts.astype(F32), axis=0) + bias
    activated = jax.nn.gelu(total, approximate=False).astype(BF)
    mine_act = copy_for_each(activated, "zl").reshape(count, half)
    activated_all = in_order(mine_act, swap(mine_act, "c"), c, 1)

    second = mm(activated_all, jnp.concatenate([w[:units] for w in w_out], axis=0))
    parts = lax.all_to_all(second.astype(BF).reshape(4, count // 4, cols), "x", 0, 0, tiled=True)
    part = jnp.sum(parts.astype(F32), axis=0)
    part = part + swap(part.astype(BF), "zh").astype(F32)
    pair_projected = (part + proj_out_bias).astype(BF)
    own = count // 8
    projected = jnp.where(zh == 0, pair_projected[:own], pair_projected[own:])
    everything = copy_for_each(pair_projected, ("g", "x")).reshape(-1, cols)

    q = jnp.arange(count, dtype=jnp.int32)
    block = ((zl + (q // own) % 4) % 4) * 2 + (c + q // (4 * own)) % 2
    at = block * own + q % own
    source, covered = seq_sources(
        image_counts, image_sequence, image_offsets, g * count + at
    )

    def gathered_place(r):
        return (r // own) % 4 * (2 * own) + (r // (4 * own)) % 2 * own + r % own

    text_place = gathered_place(at)
    column = jnp.where(
        covered,
        source // count * count + gathered_place(source % count),
        everything.shape[0] + text_place,
    )
    choose = (column[:, None] == jnp.arange(everything.shape[0] + count)[None, :]).astype(BF)
    reorder = (text_place[:, None] == q[None, :]).astype(BF)
    inputs = pick(choose, jnp.concatenate([everything, text], axis=0))
    back_rows = pick(reorder, cotangent)

    whole = jnp.concatenate(
        [mm(inputs, gate_weight), mm(inputs, up_weight), mm_t(back_rows, down_weight)], axis=1
    )
    there = swap(whole[4 * own :].astype(BF), "c")
    near = whole[: 4 * own] + there.astype(F32)
    near_sent = near.astype(BF)
    total = near[:own]
    for k in (1, 2, 3):
        total = total + from_next(near_sent[own * ((4 - k) % 4) : own * ((4 - k) % 4 + 1)], "zl", k).astype(F32)
    gate_grad, up_grad = unit_grads(
        total[:, :width], total[:, width : 2 * width], total[:, 2 * width :]
    )

    grads = jnp.concatenate([gate_grad, up_grad], axis=1)
    line = jnp.concatenate([grads] + [from_next(grads, "zl", k) for k in (1, 2, 3)], axis=0)
    other = swap(line, "c")
    halves = [
        mm_t(h[:, :width], gate_weight) + mm_t(h[:, width:], up_weight) for h in (line, other)
    ]
    turned = jnp.concatenate(halves, axis=0).astype(BF)
    restore = (q[:, None] == text_place[None, :]).astype(BF)
    ordered = pick(restore, turned)
    parts = lax.all_to_all(ordered.reshape(4, count // 4, cols), "x", 0, 0, tiled=True)
    part = jnp.sum(parts.astype(F32), axis=0)
    pair_grads = (part + swap(part.astype(BF), "zh").astype(F32)).astype(BF)
    sequence_grads = jnp.where(zh == 0, pair_grads[:own], pair_grads[own:])

    column_rows = copy_for_each(pair_grads, "g").reshape(-1, cols)
    r = jnp.arange(4 * own, dtype=jnp.int32)
    target, valid = image_targets(
        image_counts, image_sequence, image_offsets, g * count + zh * (4 * own) + r
    )
    held = valid & ((target // own) % 4 == x)
    spot = target // count * (2 * own) + (target // (4 * own)) % 2 * own + target % own
    give = (held[:, None] & (spot[:, None] == q[None, :])).astype(BF)
    parts = lax.all_to_all(pick(give, column_rows).reshape(4, own, cols), "x", 0, 0, tiled=True)
    row_grads = jnp.sum(parts.astype(F32), axis=0).astype(BF)
    return (projected, sequence_grads, row_grads)


def solution(mesh):
    finer = Mesh(mesh.devices.reshape(4, 4, 2, 2, 4), ("g", "zl", "c", "zh", "x"))
    in_specs = (
        P(ROWS, DP),
        P(DP),
        P(DP),
        P(DP, ROWS),
        P(ROWS),
        P(ROWS, DP),
        P(DP),
        P(ROWS, DP),
        P(ROWS, DP),
        P(DP, MP),
        P(DP, MP),
        P(MP, DP),
        P(),
        P(),
        P(),
    )
    out_specs = (P(ROWS, DP), P(ROWS, DP), P(ROWS, DP))
    return jax.shard_map(local, mesh=finer, in_specs=in_specs, out_specs=out_specs, check_vma=False)
```

```python
import jax
import jax.numpy as jnp
from jax import lax
from jax.experimental import pallas as pl
from jax.experimental.pallas import tpu as pltpu
from jax.sharding import Mesh
from jax.sharding import PartitionSpec as P


TOK_DEV = 128
ROWS = ("g", "zh", "x")
DP = ("zl", "c")
MP = ("zh", "x")
BF = jnp.bfloat16
F32 = jnp.float32


def from_next(value, axis, k):
    n = lax.axis_size(axis)
    return lax.ppermute(value, axis, [((i + k) % n, i) for i in range(n)])


def swap(value, axis):
    return lax.ppermute(value, axis, [(0, 1), (1, 0)])


def copy_for_each(shard, axis):
    count = lax.axis_size(axis)
    return lax.all_to_all(
        jnp.broadcast_to(shard[None], (count, *shard.shape)), axis, 0, 0, tiled=True
    )


def in_order(own, other, index, dim=0):
    return jnp.where(
        index == 0,
        jnp.concatenate([own, other], axis=dim),
        jnp.concatenate([other, own], axis=dim),
    )


def mm(a, b):
    return jnp.dot(a, b, preferred_element_type=F32)


def mm_t(a, b):
    return lax.dot_general(a, b, (((1,), (1,)), ((), ())), preferred_element_type=F32)


def pick(onehot, rows):
    return mm(onehot, rows).astype(BF)


def three_parts(v):
    hi = lax.reduce_precision(v, 8, 7)
    mid = lax.reduce_precision(v - hi, 8, 7)
    low = v - hi - mid
    return jnp.stack([hi, mid, low]).astype(BF)


def seq_sources(counts, sequence, offsets, rows):
    starts = jnp.cumsum(counts) - counts
    seq = rows // TOK_DEV
    pos = rows % TOK_DEV
    hit = (
        (sequence[None, :] == seq[:, None])
        & (offsets[None, :] <= pos[:, None])
        & (pos[:, None] < (offsets + counts)[None, :])
    )
    source = jnp.sum(jnp.where(hit, starts[None, :] + pos[:, None] - offsets[None, :], 0), axis=1)
    return (source, jnp.any(hit, axis=1))


def image_targets(counts, sequence, offsets, rows):
    starts = jnp.cumsum(counts) - counts
    hit = (starts[None, :] <= rows[:, None]) & (rows[:, None] < (starts + counts)[None, :])
    target = jnp.sum(
        jnp.where(
            hit, sequence[None, :] * TOK_DEV + offsets[None, :] + rows[:, None] - starts[None, :], 0
        ),
        axis=1,
    )
    return (target, jnp.any(hit, axis=1))


def unit_grads(gate, up, hidden_grad):
    sig = jax.nn.sigmoid(gate)
    gate_grad = (hidden_grad * up * sig * (1.0 + gate * (1.0 - sig))).astype(BF)
    up_grad = (hidden_grad * gate * sig).astype(BF)
    return (gate_grad, up_grad)


def split3(v, axis=0):
    hi = lax.reduce_precision(v, 8, 7)
    mid = lax.reduce_precision(v - hi, 8, 7)
    return jnp.concatenate([hi, mid, v - hi - mid], axis=axis).astype(BF)


def row_share(whole, own):
    there = swap(whole[4 * own :], "c")
    near = whole[: 4 * own] + there
    sent = near[own:].astype(BF)
    total = near[:own]
    for k in (1, 2, 3):
        total = total + from_next(sent[own * (3 - k) : own * (4 - k)], "zl", k).astype(F32)
    return total


def first_kernel(c_ref, x_ref, gain_ref, bias_ref, w0, w1, w2, w3, keep_ref, send_ref, z_ref):
    count, feats = x_ref.shape
    units = w0.shape[1]
    half = 2 * units
    x = x_ref[...].astype(F32)
    mean = jnp.sum(x, axis=1, keepdims=True) * (1.0 / feats)
    centred = x - mean
    spread = jnp.sum(centred * centred, axis=1, keepdims=True) * (1.0 / feats)
    gain = gain_ref[...]
    z_ref[:count, :] = (centred * gain).astype(BF)
    bias = bias_ref[...]
    extra = []
    for v in (gain, bias):
        for _ in range(3):
            part = v.astype(BF).astype(F32)
            extra.append(part)
            v = v - part
    extra.append(jnp.zeros((10, feats), F32))
    z_ref[count:, :] = jnp.concatenate(extra, axis=0).astype(BF)
    lane = lax.broadcasted_iota(jnp.int32, (count, units), 1)
    stats = jnp.where(lane == 0, mean, jnp.where(lane == 1, spread, 0.0))
    for ref in (keep_ref, send_ref):
        ref[:count, half:] = stats
        ref[count:, half:] = jnp.zeros((16, units), F32)
    z = z_ref[...]
    low = c_ref[0] == 0
    for k, w in enumerate((w0, w1, w2, w3)):
        p = jnp.dot(z, w[...], preferred_element_type=F32)
        at = (k % 2) * units
        here, there = (keep_ref, send_ref) if k < 2 else (send_ref, keep_ref)

        @pl.when(low)
        def _():
            here[:, at : at + units] = p

        @pl.when(jnp.logical_not(low))
        def _():
            there[:, at : at + units] = p


VMEM = pl.BlockSpec(memory_space=pltpu.VMEM)
SMEM = pl.BlockSpec(memory_space=pltpu.SMEM)


def first_layer(rows, gain, bias, w_in, c_ref):
    count, feats = rows.shape
    units = w_in[0].shape[1]
    shape = (count + 16, 3 * units)
    return pl.pallas_call(
        first_kernel,
        out_shape=[jax.ShapeDtypeStruct(shape, F32)] * 2,
        in_specs=[SMEM] + [VMEM] * 7,
        out_specs=[VMEM, VMEM],
        scratch_shapes=[pltpu.VMEM((count + 16, feats), BF)],
        compiler_params=pltpu.CompilerParams(vmem_limit_bytes=32 << 20),
        cost_estimate=pl.CostEstimate(
            flops=2 * count * feats * 4 * units, bytes_accessed=4 << 20, transcendentals=0
        ),
        name="first_layer",
    )(c_ref, rows, gain.reshape(1, -1), bias.reshape(1, -1), *w_in)


def second_kernel(c_ref, own_ref, other_ref, w0, w1, w2, w3, out_ref):
    units = w0.shape[0] - 16
    ws = (w0, w1, w2, w3)
    low = c_ref[0] == 0
    for lead, cond in ((0, low), (2, jnp.logical_not(low))):

        @pl.when(cond)
        def _():
            total = jnp.zeros(out_ref.shape, F32)
            for j in range(4):
                act = own_ref if j < 2 else other_ref
                a = act[:, (j % 2) * units : (j % 2 + 1) * units]
                total += jnp.dot(a, ws[(lead + j) % 4][:units, :], preferred_element_type=F32)
            out_ref[...] = total.astype(out_ref.dtype)


def second_layer(own, other, w_out, c_ref):
    count = own.shape[0]
    cols = w_out[0].shape[1]
    return pl.pallas_call(
        second_kernel,
        out_shape=jax.ShapeDtypeStruct((count, cols), BF),
        in_specs=[SMEM] + [VMEM] * 6,
        out_specs=VMEM,
        compiler_params=pltpu.CompilerParams(vmem_limit_bytes=16 << 20),
        cost_estimate=pl.CostEstimate(
            flops=4 * count * own.shape[1] * cols, bytes_accessed=1 << 20, transcendentals=0
        ),
        name="second_layer",
    )(c_ref, own, other, *w_out)


def local(
    patches,
    norm_gain,
    norm_bias,
    proj_in,
    proj_in_bias,
    proj_out,
    proj_out_bias,
    text_rows,
    out_grads,
    gate_weight,
    up_weight,
    down_weight,
    image_counts,
    image_sequence,
    image_offsets,
):
    g, zl, c, zh, x = (lax.axis_index(a) for a in ("g", "zl", "c", "zh", "x"))
    units = proj_in.shape[1]
    width = gate_weight.shape[1]
    cols = text_rows.shape[1]
    feats = patches.shape[1]

    patch_other = swap(patches, "zh")
    w_in = [proj_in] + [from_next(proj_in, "g", k) for k in (1, 2, 3)]
    packed = jnp.concatenate(
        [proj_out, jnp.pad(three_parts(proj_in_bias), ((0, 13), (0, cols - units)))], axis=0
    )
    w_out = [packed] + [from_next(packed, "g", k) for k in (1, 2, 3)]
    pair = in_order(patches, patch_other, zh)
    rows = copy_for_each(pair, "x").reshape(-1, feats)
    count = rows.shape[0]
    own = count // 8

    side = jnp.concatenate([text_rows, out_grads], axis=1)
    side_other = swap(side, "zh")
    side_pair = in_order(side, side_other, zh)
    side_all = jnp.concatenate(
        [side_pair] + [from_next(side_pair, "x", k) for k in (1, 2, 3)], axis=0
    )
    text, cotangent = side_all[:, :cols], side_all[:, cols:]

    half = 2 * units
    c_ref = c.reshape(1).astype(jnp.int32)
    keep, send = first_layer(rows, norm_gain, norm_bias, w_in, c_ref)
    near = swap(send, "c")
    mean_a, spread_a = keep[:count, half : half + 1], keep[:count, half + 1 : half + 2]
    mean_b, spread_b = near[:count, half : half + 1], near[:count, half + 1 : half + 2]
    gain_a = jnp.sum(keep[count : count + 3, :half], axis=0, keepdims=True)
    gain_b = jnp.sum(near[count : count + 3, :half], axis=0, keepdims=True)
    shift = jnp.sum((keep + near)[count + 3 : count + 6, :half], axis=0, keepdims=True)
    apart = 0.5 * (mean_a - mean_b)
    mean = 0.5 * (mean_a + mean_b)
    spread = 0.5 * (spread_a + spread_b) + apart * apart
    summed = keep[:count, :half] + near[:count, :half] + apart * (gain_a - gain_b)
    tail = jnp.concatenate([split3(gain_a + gain_b), split3(shift)], axis=0)
    stats = jnp.concatenate([split3(mean, 1), split3(spread, 1)], axis=1)
    upper = jnp.concatenate([summed.astype(BF), jnp.pad(stats, ((0, 0), (0, units - 6)))], axis=1)
    lower = jnp.broadcast_to(jnp.pad(tail, ((0, 10), (0, units)))[None], (4, 16, half + units))
    message = jnp.concatenate([upper.reshape(4, count // 4, half + units), lower], axis=1)
    parts = lax.all_to_all(message, "zl", 0, 0, tiled=True).astype(F32)
    n = count // 4
    means = jnp.sum(parts[:, :n, half : half + 3], axis=2, keepdims=True)
    spreads = jnp.sum(parts[:, :n, half + 3 : half + 6], axis=2, keepdims=True)
    gains = jnp.sum(parts[:, n : n + 3, :half], axis=1, keepdims=True)
    shift = jnp.sum(parts[:, n + 3 : n + 6, :half], axis=(0, 1))
    mean = jnp.mean(means, axis=0, keepdims=True)
    spread = jnp.mean(spreads + (means - mean) * (means - mean), axis=0)
    total = jnp.sum(parts[:, :n, :half] + (means - mean) * gains, axis=0)
    bias = jnp.concatenate(
        [jnp.sum(w[units : units + 3, :units].astype(F32), axis=0) for w in w_out]
    )
    bias = jnp.where(c == 0, bias[:half], bias[half:])
    total = total * lax.rsqrt(spread + 1e-05) + (shift + bias)
    activated = jax.nn.gelu(total, approximate=False).astype(BF)
    act_own = copy_for_each(activated, "zl").reshape(count, half)
    act_other = swap(act_own, "c")

    second = second_layer(act_own, act_other, w_out, c_ref)
    parts = lax.all_to_all(second.reshape(4, count // 4, cols), "x", 0, 0, tiled=True)
    part = jnp.sum(parts.astype(F32), axis=0)
    part = part + swap(part.astype(BF), "zh").astype(F32)
    pair_projected = (part + proj_out_bias).astype(BF)
    projected = jnp.where(zh == 0, pair_projected[:own], pair_projected[own:])
    everything = copy_for_each(pair_projected, ("g", "x")).reshape(-1, cols)

    q = jnp.arange(count, dtype=jnp.int32)
    block = ((zl + (q // own) % 4) % 4) * 2 + (c + q // (4 * own)) % 2
    at = block * own + q % own
    source, covered = seq_sources(
        image_counts, image_sequence, image_offsets, g * count + at
    )

    def gathered_place(r):
        return (r // own) % 4 * (2 * own) + (r // (4 * own)) % 2 * own + r % own

    place = gathered_place(at)
    text_place = (place - x * (2 * own)) % count
    column = jnp.where(
        covered,
        source // count * count + gathered_place(source % count),
        everything.shape[0] + text_place,
    )
    choose = (column[:, None] == jnp.arange(everything.shape[0] + count)[None, :]).astype(BF)
    reorder = (text_place[:, None] == q[None, :]).astype(BF)
    inputs = pick(choose, jnp.concatenate([everything, text], axis=0))
    back_rows = pick(reorder, cotangent)

    hidden = mm_t(back_rows, down_weight)
    hidden_grad = row_share(hidden, own)
    whole = jnp.concatenate([mm(inputs, gate_weight), mm(inputs, up_weight)], axis=1)
    total = row_share(whole, own)
    gate_grad, up_grad = unit_grads(total[:, :width], total[:, width:], hidden_grad)

    grads = jnp.concatenate([gate_grad, up_grad], axis=1)
    line = jnp.concatenate([grads] + [from_next(grads, "zl", k) for k in (1, 2, 3)], axis=0)
    other = swap(line, "c")
    halves = [
        mm_t(h[:, :width], gate_weight) + mm_t(h[:, width:], up_weight) for h in (line, other)
    ]
    turned = jnp.concatenate(halves, axis=0).astype(BF)
    restore = (q[:, None] == place[None, :]).astype(BF)
    ordered = pick(restore, turned)
    parts = lax.all_to_all(ordered.reshape(4, count // 4, cols), "x", 0, 0, tiled=True)
    part = jnp.sum(parts.astype(F32), axis=0)
    pair_grads = (part + swap(part.astype(BF), "zh").astype(F32)).astype(BF)
    sequence_grads = jnp.where(zh == 0, pair_grads[:own], pair_grads[own:])

    column_rows = copy_for_each(pair_grads, "g").reshape(-1, cols)
    r = jnp.arange(4 * own, dtype=jnp.int32)
    target, valid = image_targets(
        image_counts, image_sequence, image_offsets, g * count + zh * (4 * own) + r
    )
    held = valid & ((target // own) % 4 == x)
    spot = target // count * (2 * own) + (target // (4 * own)) % 2 * own + target % own
    give = (held[:, None] & (spot[:, None] == q[None, :])).astype(BF)
    parts = lax.all_to_all(pick(give, column_rows).reshape(4, own, cols), "x", 0, 0, tiled=True)
    row_grads = jnp.sum(parts.astype(F32), axis=0).astype(BF)
    return (projected, sequence_grads, row_grads)


def solution(mesh):
    finer = Mesh(mesh.devices.reshape(4, 4, 2, 2, 4), ("g", "zl", "c", "zh", "x"))
    in_specs = (
        P(ROWS, DP),
        P(DP),
        P(DP),
        P(DP, ROWS),
        P(ROWS),
        P(ROWS, DP),
        P(DP),
        P(ROWS, DP),
        P(ROWS, DP),
        P(DP, MP),
        P(DP, MP),
        P(MP, DP),
        P(),
        P(),
        P(),
    )
    out_specs = (P(ROWS, DP), P(ROWS, DP), P(ROWS, DP))
    return jax.shard_map(local, mesh=finer, in_specs=in_specs, out_specs=out_specs, check_vma=False)
```

```python
import jax
import jax.numpy as jnp
from jax import lax
from jax.experimental import pallas as pl
from jax.experimental.pallas import tpu as pltpu
from jax.sharding import Mesh
from jax.sharding import PartitionSpec as P


TOK_DEV = 128
ROWS = ("g", "zh", "x")
DP = ("zl", "c")
MP = ("zh", "x")
BF = jnp.bfloat16
F32 = jnp.float32


def from_next(value, axis, k):
    n = lax.axis_size(axis)
    return lax.ppermute(value, axis, [((i + k) % n, i) for i in range(n)])


def swap(value, axis):
    return lax.ppermute(value, axis, [(0, 1), (1, 0)])


def copy_for_each(shard, axis):
    count = lax.axis_size(axis)
    return lax.all_to_all(
        jnp.broadcast_to(shard[None], (count, *shard.shape)), axis, 0, 0, tiled=True
    )


def in_order(own, other, index, dim=0):
    return jnp.where(
        index == 0,
        jnp.concatenate([own, other], axis=dim),
        jnp.concatenate([other, own], axis=dim),
    )


def mm(a, b):
    return jnp.dot(a, b, preferred_element_type=F32)


def mm_t(a, b):
    return lax.dot_general(a, b, (((1,), (1,)), ((), ())), preferred_element_type=F32)


def pick(onehot, rows):
    return mm(onehot, rows).astype(BF)


def three_parts(v):
    hi = lax.reduce_precision(v, 8, 7)
    mid = lax.reduce_precision(v - hi, 8, 7)
    low = v - hi - mid
    return jnp.stack([hi, mid, low]).astype(BF)


def seq_sources(counts, sequence, offsets, rows):
    starts = jnp.cumsum(counts) - counts
    seq = rows // TOK_DEV
    pos = rows % TOK_DEV
    hit = (
        (sequence[None, :] == seq[:, None])
        & (offsets[None, :] <= pos[:, None])
        & (pos[:, None] < (offsets + counts)[None, :])
    )
    covered = jnp.any(hit, axis=1)
    source = lax.optimization_barrier(
        jnp.sum(jnp.where(hit, starts[None, :] + pos[:, None] - offsets[None, :], 0), axis=1)
    )
    return (source, covered)


def image_targets(counts, sequence, offsets, rows):
    starts = jnp.cumsum(counts) - counts
    hit = (starts[None, :] <= rows[:, None]) & (rows[:, None] < (starts + counts)[None, :])
    target = jnp.sum(
        jnp.where(
            hit, sequence[None, :] * TOK_DEV + offsets[None, :] + rows[:, None] - starts[None, :], 0
        ),
        axis=1,
    )
    return (target, jnp.any(hit, axis=1))


def unit_grads(gate, up, hidden_grad):
    sig = jax.nn.sigmoid(gate)
    gate_grad = (hidden_grad * up * sig * (1.0 + gate * (1.0 - sig))).astype(BF)
    up_grad = (hidden_grad * gate * sig).astype(BF)
    return (gate_grad, up_grad)


def split3(v, axis=0):
    hi = lax.reduce_precision(v, 8, 7)
    mid = lax.reduce_precision(v - hi, 8, 7)
    return jnp.concatenate([hi, mid, v - hi - mid], axis=axis).astype(BF)


def row_share(kept, given, own):
    there = swap(given, "c")
    near = kept + there
    sent = near[own:].astype(BF)
    total = near[:own]
    for k in (1, 2, 3):
        total = total + from_next(sent[own * (3 - k) : own * (4 - k)], "zl", k).astype(F32)
    return total


def first_kernel(c_ref, x_ref, gain_ref, bias_ref, w0, w1, w2, w3, keep_ref, send_ref, z_ref):
    count, feats = x_ref.shape
    units = w0.shape[1]
    half = 2 * units
    x = x_ref[...].astype(F32)
    mean = jnp.sum(x, axis=1, keepdims=True) * (1.0 / feats)
    centred = x - mean
    spread = jnp.sum(centred * centred, axis=1, keepdims=True) * (1.0 / feats)
    gain = gain_ref[...]
    z_ref[:count, :] = (centred * gain).astype(BF)
    bias = bias_ref[...]
    extra = []
    for v in (gain, bias):
        for _ in range(3):
            part = v.astype(BF).astype(F32)
            extra.append(part)
            v = v - part
    extra.append(jnp.zeros((10, feats), F32))
    z_ref[count:, :] = jnp.concatenate(extra, axis=0).astype(BF)
    lane = lax.broadcasted_iota(jnp.int32, (count, units), 1)
    stats = jnp.where(lane == 0, mean, jnp.where(lane == 1, spread, 0.0))
    for ref in (keep_ref, send_ref):
        ref[:count, half:] = stats
        ref[count:, half:] = jnp.zeros((16, units), F32)
    z = z_ref[...]
    low = c_ref[0] == 0
    for k, w in enumerate((w0, w1, w2, w3)):
        p = jnp.dot(z, w[...], preferred_element_type=F32)
        at = (k % 2) * units
        here, there = (keep_ref, send_ref) if k < 2 else (send_ref, keep_ref)

        @pl.when(low)
        def _():
            here[:, at : at + units] = p

        @pl.when(jnp.logical_not(low))
        def _():
            there[:, at : at + units] = p


VMEM = pl.BlockSpec(memory_space=pltpu.VMEM)
SMEM = pl.BlockSpec(memory_space=pltpu.SMEM)


def first_layer(rows, gain, bias, w_in, c_ref):
    count, feats = rows.shape
    units = w_in[0].shape[1]
    shape = (count + 16, 3 * units)
    return pl.pallas_call(
        first_kernel,
        out_shape=[jax.ShapeDtypeStruct(shape, F32)] * 2,
        in_specs=[SMEM] + [VMEM] * 7,
        out_specs=[VMEM, VMEM],
        scratch_shapes=[pltpu.VMEM((count + 16, feats), BF)],
        compiler_params=pltpu.CompilerParams(vmem_limit_bytes=32 << 20),
        cost_estimate=pl.CostEstimate(
            flops=2 * count * feats * 4 * units, bytes_accessed=4 << 20, transcendentals=0
        ),
        name="first_layer",
    )(c_ref, rows, gain.reshape(1, -1), bias.reshape(1, -1), *w_in)


def second_kernel(c_ref, own_ref, other_ref, w0, w1, w2, w3, out_ref):
    units = w0.shape[0] - 16
    ws = (w0, w1, w2, w3)
    low = c_ref[0] == 0
    for lead, cond in ((0, low), (2, jnp.logical_not(low))):

        @pl.when(cond)
        def _():
            total = jnp.zeros(out_ref.shape, F32)
            for j in range(4):
                act = own_ref if j < 2 else other_ref
                a = act[:, (j % 2) * units : (j % 2 + 1) * units]
                total += jnp.dot(a, ws[(lead + j) % 4][:units, :], preferred_element_type=F32)
            out_ref[...] = total.astype(out_ref.dtype)


def second_layer(own, other, w_out, c_ref):
    count = own.shape[0]
    cols = w_out[0].shape[1]
    return pl.pallas_call(
        second_kernel,
        out_shape=jax.ShapeDtypeStruct((count, cols), BF),
        in_specs=[SMEM] + [VMEM] * 6,
        out_specs=VMEM,
        compiler_params=pltpu.CompilerParams(vmem_limit_bytes=16 << 20),
        cost_estimate=pl.CostEstimate(
            flops=4 * count * own.shape[1] * cols, bytes_accessed=1 << 20, transcendentals=0
        ),
        name="second_layer",
    )(c_ref, own, other, *w_out)


def local(
    patches,
    norm_gain,
    norm_bias,
    proj_in,
    proj_in_bias,
    proj_out,
    proj_out_bias,
    text_rows,
    out_grads,
    gate_weight,
    up_weight,
    down_weight,
    image_counts,
    image_sequence,
    image_offsets,
):
    g, zl, c, zh, x = (lax.axis_index(a) for a in ("g", "zl", "c", "zh", "x"))
    units = proj_in.shape[1]
    width = gate_weight.shape[1]
    cols = text_rows.shape[1]
    feats = patches.shape[1]

    patch_other = swap(patches, "zh")
    w_in = [proj_in] + [from_next(proj_in, "g", k) for k in (1, 2, 3)]
    packed = jnp.concatenate(
        [proj_out, jnp.pad(three_parts(proj_in_bias), ((0, 13), (0, cols - units)))], axis=0
    )
    w_out = [packed] + [from_next(packed, "g", k) for k in (1, 2, 3)]
    pair = in_order(patches, patch_other, zh)
    rows = copy_for_each(pair, "x").reshape(-1, feats)
    count = rows.shape[0]
    own = count // 8

    side = jnp.concatenate([text_rows, out_grads], axis=1)
    side_other = swap(side, "zh")
    side_pair = in_order(side, side_other, zh)
    side_all = jnp.concatenate(
        [side_pair] + [from_next(side_pair, "x", k) for k in (1, 2, 3)], axis=0
    )
    text, cotangent = side_all[:, :cols], side_all[:, cols:]

    half = 2 * units
    c_ref = c.reshape(1).astype(jnp.int32)
    keep, send = first_layer(rows, norm_gain, norm_bias, w_in, c_ref)
    near = swap(send, "c")
    mean_a, spread_a = keep[:count, half : half + 1], keep[:count, half + 1 : half + 2]
    mean_b, spread_b = near[:count, half : half + 1], near[:count, half + 1 : half + 2]
    gain_a = jnp.sum(keep[count : count + 3, :half], axis=0, keepdims=True)
    gain_b = jnp.sum(near[count : count + 3, :half], axis=0, keepdims=True)
    shift = jnp.sum((keep + near)[count + 3 : count + 6, :half], axis=0, keepdims=True)
    apart = 0.5 * (mean_a - mean_b)
    mean = 0.5 * (mean_a + mean_b)
    spread = 0.5 * (spread_a + spread_b) + apart * apart
    summed = keep[:count, :half] + near[:count, :half] + apart * (gain_a - gain_b)
    tail = jnp.concatenate([split3(gain_a + gain_b), split3(shift)], axis=0)
    stats = jnp.concatenate([split3(mean, 1), split3(spread, 1)], axis=1)
    upper = jnp.concatenate([summed.astype(BF), jnp.pad(stats, ((0, 0), (0, units - 6)))], axis=1)
    lower = jnp.broadcast_to(jnp.pad(tail, ((0, 10), (0, units)))[None], (4, 16, half + units))
    message = jnp.concatenate([upper.reshape(4, count // 4, half + units), lower], axis=1)
    parts = lax.all_to_all(message, "zl", 0, 0, tiled=True).astype(F32)
    n = count // 4
    means = jnp.sum(parts[:, :n, half : half + 3], axis=2, keepdims=True)
    spreads = jnp.sum(parts[:, :n, half + 3 : half + 6], axis=2, keepdims=True)
    gains = jnp.sum(parts[:, n : n + 3, :half], axis=1, keepdims=True)
    shift = jnp.sum(parts[:, n + 3 : n + 6, :half], axis=(0, 1))
    mean = jnp.mean(means, axis=0, keepdims=True)
    spread = jnp.mean(spreads + (means - mean) * (means - mean), axis=0)
    total = jnp.sum(parts[:, :n, :half] + (means - mean) * gains, axis=0)
    bias = jnp.concatenate(
        [jnp.sum(w[units : units + 3, :units].astype(F32), axis=0) for w in w_out]
    )
    bias = jnp.where(c == 0, bias[:half], bias[half:])
    total = total * lax.rsqrt(spread + 1e-05) + (shift + bias)
    activated = jax.nn.gelu(total, approximate=False).astype(BF)
    act_own = copy_for_each(activated, "zl").reshape(count, half)
    act_other = swap(act_own, "c")

    second = second_layer(act_own, act_other, w_out, c_ref)
    parts = lax.all_to_all(second.reshape(4, count // 4, cols), "x", 0, 0, tiled=True)
    part = jnp.sum(parts.astype(F32), axis=0)
    part = part + swap(part.astype(BF), "zh").astype(F32)
    pair_projected = (part + proj_out_bias).astype(BF)
    projected = jnp.where(zh == 0, pair_projected[:own], pair_projected[own:])
    line_rows = jnp.concatenate(
        [pair_projected] + [from_next(pair_projected, "x", k) for k in (1, 2, 3)], axis=0
    )
    far_rows = [from_next(line_rows, "g", k) for k in (1, 2, 3)]

    q = jnp.arange(count, dtype=jnp.int32)
    block = ((zl + (q // own) % 4) % 4) * 2 + (c + q // (4 * own)) % 2
    at = block * own + q % own
    source, covered = seq_sources(image_counts, image_sequence, image_offsets, g * count + at)

    def gathered_place(r):
        return (r // own) % 4 * (2 * own) + (r // (4 * own)) % 2 * own + r % own

    place = gathered_place(at)

    def x_turned(p):
        return (p - x * (2 * own)) % count

    text_place = x_turned(place)
    column = jnp.where(
        covered,
        (source // count - g) % 4 * count + x_turned(gathered_place(source % count)),
        4 * count + text_place,
    )
    column = lax.optimization_barrier(column)
    choose = column[:, None]
    near_choice = jnp.concatenate([choose == q[None, :], choose == q[None, :] + 4 * count], axis=1)
    far_choice = choose == count + jnp.arange(3 * count)[None, :]
    near_inputs = mm(near_choice.astype(BF), jnp.concatenate([line_rows, text], axis=0))
    far_inputs = mm(far_choice.astype(BF), jnp.concatenate(far_rows, axis=0))
    inputs = (near_inputs + far_inputs).astype(BF)
    reorder = (text_place[:, None] == q[None, :]).astype(BF)
    back_rows = pick(reorder, cotangent)

    hidden = [mm_t(back_rows[k : k + 4 * own], down_weight) for k in (0, 4 * own)]
    hidden_grad = row_share(*hidden, own)
    whole = jnp.concatenate([mm(inputs, gate_weight), mm(inputs, up_weight)], axis=1)
    total = row_share(whole[: 4 * own], whole[4 * own :], own)
    gate_grad, up_grad = unit_grads(total[:, :width], total[:, width:], hidden_grad)

    grads = jnp.concatenate([gate_grad, up_grad], axis=1)
    line = jnp.concatenate([grads] + [from_next(grads, "zl", k) for k in (1, 2, 3)], axis=0)
    other = swap(line, "c")
    halves = [
        mm_t(h[:, :width], gate_weight) + mm_t(h[:, width:], up_weight) for h in (line, other)
    ]
    turned = jnp.concatenate(halves, axis=0).astype(BF)

    def image_rows(k):
        base = (g - k) % 4 * count
        row = base + q // (2 * own) * own + q // own % 2 * (4 * own) + q % own
        target, valid = image_targets(image_counts, image_sequence, image_offsets, row)
        held = valid & (target // count == g)
        return (held[:, None] & ((target % count)[:, None] == at[None, :])).astype(BF)

    back = []
    for k in (2, 1, 3):
        given = pick(image_rows(k), turned)
        back.append(from_next(given, "g", k))
    restore = (q[:, None] == place[None, :]).astype(BF)
    ordered = pick(restore, turned)
    image = mm(image_rows(0), turned) + sum(b.astype(F32) for b in back)
    both = jnp.concatenate(
        [ordered.reshape(4, 2 * own, cols), image.astype(BF).reshape(4, 2 * own, cols)], axis=1
    )
    parts = lax.all_to_all(both, "x", 0, 0, tiled=True)
    part = jnp.sum(parts.astype(F32), axis=0).reshape(2, 2, own, cols)
    keep = jnp.where(zh == 0, part[:, 0], part[:, 1])
    give = jnp.where(zh == 0, part[:, 1], part[:, 0]).astype(BF)
    final = (keep + swap(give, "zh").astype(F32)).astype(BF)
    sequence_grads, row_grads = final[0], final[1]
    return (projected, sequence_grads, row_grads)


def solution(mesh):
    finer = Mesh(mesh.devices.reshape(4, 4, 2, 2, 4), ("g", "zl", "c", "zh", "x"))
    in_specs = (
        P(ROWS, DP),
        P(DP),
        P(DP),
        P(DP, ROWS),
        P(ROWS),
        P(ROWS, DP),
        P(DP),
        P(ROWS, DP),
        P(ROWS, DP),
        P(DP, MP),
        P(DP, MP),
        P(MP, DP),
        P(),
        P(),
        P(),
    )
    out_specs = (P(ROWS, DP), P(ROWS, DP), P(ROWS, DP))
    return jax.shard_map(local, mesh=finer, in_specs=in_specs, out_specs=out_specs, check_vma=False)
```

```python
import jax
import jax.numpy as jnp
from jax import lax
from jax.experimental import pallas as pl
from jax.experimental.pallas import tpu as pltpu
from jax.sharding import Mesh
from jax.sharding import PartitionSpec as P


TOK_DEV = 128
ROWS = ("g", "zh", "x")
DP = ("zl", "c")
MP = ("zh", "x")
BF = jnp.bfloat16
F32 = jnp.float32


def from_next(value, axis, k):
    n = lax.axis_size(axis)
    return lax.ppermute(value, axis, [((i + k) % n, i) for i in range(n)])


def swap(value, axis):
    return lax.ppermute(value, axis, [(0, 1), (1, 0)])


def in_order(own, other, index, dim=0):
    return jnp.where(
        index == 0,
        jnp.concatenate([own, other], axis=dim),
        jnp.concatenate([other, own], axis=dim),
    )


def line_of(value, axis):
    return [value] + [from_next(value, axis, k) for k in (1, 2, 3)]


def mm(a, b):
    return jnp.dot(a, b, preferred_element_type=F32)


def mm_t(a, b):
    return lax.dot_general(a, b, (((1,), (1,)), ((), ())), preferred_element_type=F32)


def pick(onehot, rows):
    return mm(onehot, rows).astype(BF)


def three_parts(v):
    hi = lax.reduce_precision(v, 8, 7)
    mid = lax.reduce_precision(v - hi, 8, 7)
    low = v - hi - mid
    return jnp.stack([hi, mid, low]).astype(BF)


def seq_sources(counts, sequence, offsets, rows):
    starts = jnp.cumsum(counts) - counts
    seq = rows // TOK_DEV
    pos = rows % TOK_DEV
    hit = (
        (sequence[None, :] == seq[:, None])
        & (offsets[None, :] <= pos[:, None])
        & (pos[:, None] < (offsets + counts)[None, :])
    )
    covered = jnp.any(hit, axis=1)
    source = lax.optimization_barrier(
        jnp.sum(jnp.where(hit, starts[None, :] + pos[:, None] - offsets[None, :], 0), axis=1)
    )
    return (source, covered)


def image_targets(counts, sequence, offsets, rows):
    starts = jnp.cumsum(counts) - counts
    hit = (starts[None, :] <= rows[:, None]) & (rows[:, None] < (starts + counts)[None, :])
    target = jnp.sum(
        jnp.where(
            hit, sequence[None, :] * TOK_DEV + offsets[None, :] + rows[:, None] - starts[None, :], 0
        ),
        axis=1,
    )
    return (target, jnp.any(hit, axis=1))


def unit_grads(gate, up, hidden_grad):
    sig = jax.nn.sigmoid(gate)
    gate_grad = (hidden_grad * up * sig * (1.0 + gate * (1.0 - sig))).astype(BF)
    up_grad = (hidden_grad * gate * sig).astype(BF)
    return (gate_grad, up_grad)


def row_share(kept, given, own):
    there = swap(given, "c")
    near = kept + there
    sent = near[own:].astype(BF)
    total = near[:own]
    for k in (1, 2, 3):
        total = total + from_next(sent[own * (3 - k) : own * (4 - k)], "zl", k).astype(F32)
    return total


VMEM = pl.BlockSpec(memory_space=pltpu.VMEM)
SMEM = pl.BlockSpec(memory_space=pltpu.SMEM)
ANY = pl.BlockSpec(memory_space=pl.ANY)


def first_kernel(
    c_ref, x0, x1, x2, x3, gain_ref, bias_ref, w0, w1, w2, w3, keep_ref, send_ref, z_ref, w_ref, sems
):
    n, feats = x0.shape
    count = 4 * n
    units = w0.shape[1]
    half = 2 * units
    copies = [
        pltpu.make_async_copy(w, w_ref.at[:, pl.ds(k * units, units)], sems.at[k])
        for k, w in enumerate((w0, w1, w2, w3))
    ]
    for copy in copies:
        copy.start()
    gain = gain_ref[...]
    lane = lax.broadcasted_iota(jnp.int32, (n, units), 1)
    for k, x_ref in enumerate((x0, x1, x2, x3)):
        x = x_ref[...].astype(F32)
        mean = jnp.sum(x, axis=1, keepdims=True) * (1.0 / feats)
        centred = x - mean
        spread = jnp.sum(centred * centred, axis=1, keepdims=True) * (1.0 / feats)
        z_ref[k * n : (k + 1) * n, :] = (centred * gain).astype(BF)
        stats = jnp.where(lane == 0, mean, jnp.where(lane == 1, spread, 0.0))
        for ref in (keep_ref, send_ref):
            ref[k * n : (k + 1) * n, half:] = stats
    extra = []
    for v in (gain, bias_ref[...]):
        for _ in range(3):
            part = v.astype(BF).astype(F32)
            extra.append(part)
            v = v - part
    extra.append(jnp.zeros((10, feats), F32))
    z_ref[count:, :] = jnp.concatenate(extra, axis=0).astype(BF)
    for ref in (keep_ref, send_ref):
        ref[count:, half:] = jnp.zeros((16, units), F32)
    for copy in copies:
        copy.wait()
    p = jnp.dot(z_ref[...], w_ref[...], preferred_element_type=F32)
    low = c_ref[0] == 0
    keep_ref[:, :half] = jnp.where(low, p[:, :half], p[:, half:])
    send_ref[:, :half] = jnp.where(low, p[:, half:], p[:, :half])


def first_layer(rows, gain, bias, w_in, c_ref):
    n, feats = rows[0].shape
    count = 4 * n
    units = w_in[0].shape[1]
    shape = (count + 16, 3 * units)
    return pl.pallas_call(
        first_kernel,
        out_shape=[jax.ShapeDtypeStruct(shape, F32)] * 2,
        in_specs=[SMEM] + [VMEM] * 6 + [ANY] * 4,
        out_specs=[VMEM, VMEM],
        scratch_shapes=[
            pltpu.VMEM((count + 16, feats), BF),
            pltpu.VMEM((feats, 4 * units), BF),
            pltpu.SemaphoreType.DMA((4,)),
        ],
        compiler_params=pltpu.CompilerParams(vmem_limit_bytes=32 << 20),
        cost_estimate=pl.CostEstimate(
            flops=2 * count * feats * 4 * units, bytes_accessed=4 << 20, transcendentals=0
        ),
        name="first_layer",
    )(c_ref, *rows, gain.reshape(1, -1), bias.reshape(1, -1), *w_in)


def pieces(v):
    out = []
    for _ in range(3):
        part = v.astype(BF).astype(F32)
        out.append(part)
        v = v - part
    return out


def pair_kernel(at_ref, keep_ref, near_ref, own_ref, m1, m2, m3, row_ref):
    n = own_ref.shape[0] - 16
    count = 4 * n
    wide = own_ref.shape[1]
    half = wide * 2 // 3
    keep, near = keep_ref[:count, :half], near_ref[:count, :half]
    stats_a, stats_b = keep_ref[:count, half:], near_ref[:count, half:]
    mean_a, spread_a = stats_a[:, 0:1], stats_a[:, 1:2]
    mean_b, spread_b = stats_b[:, 0:1], stats_b[:, 1:2]
    tail_a, tail_b = keep_ref[count:, :half], near_ref[count:, :half]
    gain_a = jnp.sum(tail_a[0:3], axis=0, keepdims=True)
    gain_b = jnp.sum(tail_b[0:3], axis=0, keepdims=True)
    shift = jnp.sum(tail_a[3:6] + tail_b[3:6], axis=0, keepdims=True)
    apart = 0.5 * (mean_a - mean_b)
    mean = 0.5 * (mean_a + mean_b)
    spread = 0.5 * (spread_a + spread_b) + apart * apart
    row_ref[:, :half] = keep + near + apart * (gain_a - gain_b)
    columns = pieces(mean) + pieces(spread)
    lane = lax.broadcasted_iota(jnp.int32, (count, wide - half), 1)
    stats = jnp.zeros((count, wide - half), F32)
    for k, column in enumerate(columns):
        stats = jnp.where(lane == k, column, stats)
    row_ref[:, half:] = stats
    lower = jnp.concatenate(
        pieces(gain_a + gain_b) + pieces(shift) + [jnp.zeros((10, half), F32)], axis=0
    )
    lower = jnp.concatenate([lower, jnp.zeros((16, wide - half), F32)], axis=1)
    own_ref[:n, :] = row_ref[pl.ds(pl.multiple_of(at_ref[0], n), n), :]
    own_ref[n:, :] = lower
    for k, ref in enumerate((m1, m2, m3)):
        ref[:n, :] = row_ref[pl.ds(pl.multiple_of(at_ref[k + 1], n), n), :].astype(BF)
        ref[n:, :] = lower.astype(BF)


def pair_sum(keep, near, at):
    rows, wide = keep.shape
    n = (rows - 16) // 4
    out = (n + 16, wide)
    return pl.pallas_call(
        pair_kernel,
        out_shape=[jax.ShapeDtypeStruct(out, F32)] + [jax.ShapeDtypeStruct(out, BF)] * 3,
        in_specs=[SMEM, VMEM, VMEM],
        out_specs=[VMEM] * 4,
        scratch_shapes=[pltpu.VMEM((4 * n, wide), F32)],
        compiler_params=pltpu.CompilerParams(vmem_limit_bytes=16 << 20),
        cost_estimate=pl.CostEstimate(
            flops=10 * rows * wide, bytes_accessed=1 << 20, transcendentals=0
        ),
        name="pair_sum",
    )(at, keep, near)


def second_kernel(c_ref, at_ref, own_ref, other_ref, w0, w1, w2, w3, kept, s1, s2, s3, sum_ref):
    units = w0.shape[0] - 16
    n = kept.shape[0]
    low = c_ref[0] == 0
    total = jnp.zeros(sum_ref.shape, F32)
    for j, w in enumerate((w0, w1, w2, w3)):
        at = slice((j % 2) * units, (j % 2 + 1) * units)
        a, b = (own_ref, other_ref) if j < 2 else (other_ref, own_ref)
        act = jnp.where(low, a[:, at].astype(F32), b[:, at].astype(F32)).astype(BF)
        total += jnp.dot(act, w[:units, :], preferred_element_type=F32)
    sum_ref[...] = total
    for k, ref in enumerate((kept, s1, s2, s3)):
        ref[...] = sum_ref[pl.ds(pl.multiple_of(at_ref[k], n), n), :].astype(ref.dtype)


def second_layer(own, other, w_out, c_ref, at):
    count = own.shape[0]
    cols = w_out[0].shape[1]
    out = (count // 4, cols)
    return pl.pallas_call(
        second_kernel,
        out_shape=[jax.ShapeDtypeStruct(out, F32)] + [jax.ShapeDtypeStruct(out, BF)] * 3,
        in_specs=[SMEM, SMEM] + [VMEM] * 6,
        out_specs=[VMEM] * 4,
        scratch_shapes=[pltpu.VMEM((count, cols), F32)],
        compiler_params=pltpu.CompilerParams(vmem_limit_bytes=16 << 20),
        cost_estimate=pl.CostEstimate(
            flops=4 * count * own.shape[1] * cols, bytes_accessed=1 << 20, transcendentals=0
        ),
        name="second_layer",
    )(c_ref, at, own, other, *w_out)


def local(
    patches,
    norm_gain,
    norm_bias,
    proj_in,
    proj_in_bias,
    proj_out,
    proj_out_bias,
    text_rows,
    out_grads,
    gate_weight,
    up_weight,
    down_weight,
    image_counts,
    image_sequence,
    image_offsets,
):
    g, zl, c, zh, x = (lax.axis_index(a) for a in ("g", "zl", "c", "zh", "x"))
    units = proj_in.shape[1]
    width = gate_weight.shape[1]
    cols = text_rows.shape[1]

    patch_other = swap(patches, "zh")
    w_in = [proj_in] + [from_next(proj_in, "g", k) for k in (1, 2, 3)]
    packed = jnp.concatenate(
        [proj_out, jnp.pad(three_parts(proj_in_bias), ((0, 13), (0, cols - units)))], axis=0
    )
    w_out = [packed] + [from_next(packed, "g", k) for k in (1, 2, 3)]
    pair = in_order(patches, patch_other, zh)
    rows = line_of(pair, "x")
    own = patches.shape[0]
    count = 8 * own

    side = jnp.concatenate([text_rows, out_grads], axis=1)
    side_other = swap(side, "zh")
    side_pair = in_order(side, side_other, zh)
    side_all = jnp.concatenate(line_of(side_pair, "x"), axis=0)
    text, cotangent = side_all[:, :cols], side_all[:, cols:]

    half = 2 * units
    c_ref = c.reshape(1).astype(jnp.int32)
    keep, send = first_layer(rows, norm_gain, norm_bias, w_in, c_ref)
    near = swap(send, "c")
    turns = jnp.arange(4, dtype=jnp.int32)
    n = 2 * own
    kept, *sent = pair_sum(keep, near, (zl - turns) % 4 * n)
    parts = [kept] + [from_next(v, "zl", k + 1).astype(F32) for k, v in enumerate(sent)]
    means = [jnp.sum(p[:n, half : half + 3], axis=1, keepdims=True) for p in parts]
    spreads = [jnp.sum(p[:n, half + 3 : half + 6], axis=1, keepdims=True) for p in parts]
    gains = [jnp.sum(p[n : n + 3, :half], axis=0, keepdims=True) for p in parts]
    shift = sum(jnp.sum(p[n + 3 : n + 6, :half], axis=0) for p in parts)
    mean = sum(means) * 0.25
    spread = sum(v + (m - mean) * (m - mean) for v, m in zip(spreads, means)) * 0.25
    total = sum(p[:n, :half] + (m - mean) * w for p, m, w in zip(parts, means, gains))
    biases = [jnp.sum(w_out[0][units : units + 3, :units].astype(F32), axis=0)]
    biases += [jnp.sum(w[units : units + 3, :units].astype(F32), axis=0) for w in w_out[1:]]
    bias = jnp.concatenate(biases)
    bias = jnp.where(c == 0, bias[:half], bias[half:])
    total = total * lax.rsqrt(spread + 1e-05) + (shift + bias)
    activated = jax.nn.gelu(total, approximate=False).astype(BF)
    act_own = jnp.concatenate(line_of(activated, "zl"), axis=0)
    act_other = swap(act_own, "c")

    part, *sent = second_layer(act_own, act_other, w_out, c_ref, (-turns - zl) % 4 * n)
    for k, v in enumerate(sent):
        part = part + from_next(v, "x", k + 1).astype(F32)
    part = part + swap(part.astype(BF), "zh").astype(F32)
    pair_projected = (part + proj_out_bias).astype(BF)
    projected = jnp.where(zh == 0, pair_projected[:own], pair_projected[own:])
    line_rows = jnp.concatenate(line_of(pair_projected, "x"), axis=0)
    far_rows = [from_next(line_rows, "g", k) for k in (1, 2, 3)]

    q = jnp.arange(count, dtype=jnp.int32)
    block = ((zl + (q // own) % 4) % 4) * 2 + (c + q // (4 * own)) % 2
    at = block * own + q % own
    source, covered = seq_sources(image_counts, image_sequence, image_offsets, g * count + at)

    def gathered_place(r):
        return (r // own) % 4 * (2 * own) + (r // (4 * own)) % 2 * own + r % own

    place = gathered_place(at)

    def x_turned(p):
        return (p - x * (2 * own)) % count

    text_place = x_turned(place)
    column = jnp.where(
        covered,
        (source // count - g) % 4 * count + x_turned(gathered_place(source % count)),
        4 * count + text_place,
    )
    column = lax.optimization_barrier(column)
    choose = column[:, None]
    near_choice = jnp.concatenate([choose == q[None, :], choose == q[None, :] + 4 * count], axis=1)
    far_choice = choose == count + jnp.arange(3 * count)[None, :]
    near_inputs = mm(near_choice.astype(BF), jnp.concatenate([line_rows, text], axis=0))
    far_inputs = mm(far_choice.astype(BF), jnp.concatenate(far_rows, axis=0))
    inputs = (near_inputs + far_inputs).astype(BF)
    reorder = (text_place[:, None] == q[None, :]).astype(BF)
    back_rows = pick(reorder, cotangent)

    hidden = [mm_t(back_rows[k : k + 4 * own], down_weight) for k in (0, 4 * own)]
    hidden_grad = row_share(*hidden, own)
    whole = jnp.concatenate([mm(inputs, gate_weight), mm(inputs, up_weight)], axis=1)
    total = row_share(whole[: 4 * own], whole[4 * own :], own)
    gate_grad, up_grad = unit_grads(total[:, :width], total[:, width:], hidden_grad)

    grads = jnp.concatenate([gate_grad, up_grad], axis=1)
    line = jnp.concatenate([grads] + [from_next(grads, "zl", k) for k in (1, 2, 3)], axis=0)
    other = swap(line, "c")
    halves = [
        mm_t(h[:, :width], gate_weight) + mm_t(h[:, width:], up_weight) for h in (line, other)
    ]
    turned = jnp.concatenate(halves, axis=0).astype(BF)

    def image_rows(k):
        base = (g - k) % 4 * count
        row = base + (x - q // (2 * own)) % 4 * own + q // own % 2 * (4 * own) + q % own
        target, valid = image_targets(image_counts, image_sequence, image_offsets, row)
        held = valid & (target // count == g)
        return (held[:, None] & ((target % count)[:, None] == at[None, :])).astype(BF)

    back = []
    for k in (2, 1, 3):
        given = pick(image_rows(k), turned)
        back.append(from_next(given, "g", k))
    restore = (q[:, None] == ((x - place // n) % 4 * n + place % n)[None, :]).astype(BF)
    ordered = pick(restore, turned)
    image = mm(image_rows(0), turned) + sum(b.astype(F32) for b in back)
    image = image.astype(BF)
    both = [
        jnp.concatenate([v[k * n : (k + 1) * n] for v in (ordered, image)], axis=0)
        for k in range(4)
    ]
    part = both[0].astype(F32)
    for k in (2, 1, 3):
        part = part + from_next(both[k], "x", k).astype(F32)
    part = part.reshape(2, 2, own, cols)
    keep = jnp.where(zh == 0, part[:, 0], part[:, 1])
    give = jnp.where(zh == 0, part[:, 1], part[:, 0]).astype(BF)
    final = (keep + swap(give, "zh").astype(F32)).astype(BF)
    sequence_grads, row_grads = final[0], final[1]
    return (projected, sequence_grads, row_grads)


def solution(mesh):
    finer = Mesh(mesh.devices.reshape(4, 4, 2, 2, 4), ("g", "zl", "c", "zh", "x"))
    in_specs = (
        P(ROWS, DP),
        P(DP),
        P(DP),
        P(DP, ROWS),
        P(ROWS),
        P(ROWS, DP),
        P(DP),
        P(ROWS, DP),
        P(ROWS, DP),
        P(DP, MP),
        P(DP, MP),
        P(MP, DP),
        P(),
        P(),
        P(),
    )
    out_specs = (P(ROWS, DP), P(ROWS, DP), P(ROWS, DP))
    return jax.shard_map(local, mesh=finer, in_specs=in_specs, out_specs=out_specs, check_vma=False)
```

```python
import jax
import jax.numpy as jnp
from jax import lax
from jax.experimental import pallas as pl
from jax.experimental.pallas import tpu as pltpu
from jax.sharding import Mesh
from jax.sharding import PartitionSpec as P


TOK_DEV = 128
ROWS = ("g", "zh", "x")
DP = ("zl", "c")
MP = ("zh", "x")
BF = jnp.bfloat16
F32 = jnp.float32


def from_next(value, axis, k):
    n = lax.axis_size(axis)
    return lax.ppermute(value, axis, [((i + k) % n, i) for i in range(n)])


def swap(value, axis):
    return lax.ppermute(value, axis, [(0, 1), (1, 0)])


def copy_for_each(shard, axis):
    count = lax.axis_size(axis)
    return lax.all_to_all(
        jnp.broadcast_to(shard[None], (count, *shard.shape)), axis, 0, 0, tiled=True
    )


def in_order(own, other, index, dim=0):
    return jnp.where(
        index == 0,
        jnp.concatenate([own, other], axis=dim),
        jnp.concatenate([other, own], axis=dim),
    )


def line_of(value, axis):
    return [value] + [from_next(value, axis, k) for k in (1, 2, 3)]


def mm(a, b):
    return jnp.dot(a, b, preferred_element_type=F32)


def mm_t(a, b):
    return lax.dot_general(a, b, (((1,), (1,)), ((), ())), preferred_element_type=F32)


def pick(onehot, rows):
    return mm(onehot, rows).astype(BF)


def three_parts(v):
    hi = lax.reduce_precision(v, 8, 7)
    mid = lax.reduce_precision(v - hi, 8, 7)
    low = v - hi - mid
    return jnp.stack([hi, mid, low]).astype(BF)


def seq_sources(counts, sequence, offsets, rows):
    starts = jnp.cumsum(counts) - counts
    seq = rows // TOK_DEV
    pos = rows % TOK_DEV
    hit = (
        (sequence[None, :] == seq[:, None])
        & (offsets[None, :] <= pos[:, None])
        & (pos[:, None] < (offsets + counts)[None, :])
    )
    covered = jnp.any(hit, axis=1)
    source = lax.optimization_barrier(
        jnp.sum(jnp.where(hit, starts[None, :] + pos[:, None] - offsets[None, :], 0), axis=1)
    )
    return (source, covered)


def image_targets(counts, sequence, offsets, rows):
    starts = jnp.cumsum(counts) - counts
    hit = (starts[None, :] <= rows[:, None]) & (rows[:, None] < (starts + counts)[None, :])
    target = jnp.sum(
        jnp.where(
            hit, sequence[None, :] * TOK_DEV + offsets[None, :] + rows[:, None] - starts[None, :], 0
        ),
        axis=1,
    )
    return (target, jnp.any(hit, axis=1))


def unit_grads(gate, up, hidden_grad):
    sig = jax.nn.sigmoid(gate)
    gate_grad = (hidden_grad * up * sig * (1.0 + gate * (1.0 - sig))).astype(BF)
    up_grad = (hidden_grad * gate * sig).astype(BF)
    return (gate_grad, up_grad)


def row_share(kept, given, own):
    there = swap(given, "c")
    near = kept + there
    sent = near[own:].astype(BF)
    total = near[:own]
    for k in (1, 2, 3):
        total = total + from_next(sent[own * (3 - k) : own * (4 - k)], "zl", k).astype(F32)
    return total


VMEM = pl.BlockSpec(memory_space=pltpu.VMEM)
SMEM = pl.BlockSpec(memory_space=pltpu.SMEM)
ANY = pl.BlockSpec(memory_space=pl.ANY)


def first_kernel(
    c_ref, x0, x1, x2, x3, gain_ref, bias_ref, w0, w1, w2, w3,
    keep_ref, send_ref, out_ref, shift_ref, z_ref, w_ref, extra_ref, sems
):
    n, feats = x0.shape
    count = 4 * n
    units = w0.shape[1]
    half = 2 * units
    copies = []

    def copy(src, dst):
        copies.append(pltpu.make_async_copy(src, dst, sems.at[len(copies)]))
        copies[-1].start()

    ws = (w0, w1, w2, w3)
    for k, w in enumerate(ws):
        copy(w.at[pl.ds(0, feats)], w_ref.at[:, pl.ds(k * units, units)])
    for k, w in enumerate(ws):
        for j in range(out_ref.shape[1] // units):
            copy(
                w.at[pl.ds(feats + j * units, units)],
                out_ref.at[pl.ds(k * units, units), pl.ds(j * units, units)],
            )
        copy(w.at[pl.ds(w.shape[0] - 16, 16)], extra_ref.at[:, pl.ds(k * units, units)])
    gain = gain_ref[...]
    step = 16
    lane = lax.broadcasted_iota(jnp.int32, (step, units), 1)
    for k, x_ref in enumerate((x0, x1, x2, x3)):

        @pl.loop(0, n // step)
        def _(i):
            x = x_ref[pl.ds(pl.multiple_of(i * step, step), step), :].astype(F32)
            mean = jnp.sum(x, axis=1, keepdims=True) * (1.0 / feats)
            centred = x - mean
            spread = jnp.sum(centred * centred, axis=1, keepdims=True) * (1.0 / feats)
            rows = pl.ds(pl.multiple_of(k * n + i * step, step), step)
            z_ref[rows, :] = (centred * gain).astype(BF)
            stats = jnp.where(lane == 0, mean, jnp.where(lane == 1, spread, 0.0))
            for ref in (keep_ref, send_ref):
                ref[rows, half:] = stats

    extra = []
    for v in (gain, bias_ref[...]):
        extra += pieces(v)
    extra.append(jnp.zeros((10, feats), F32))
    z_ref[count:, :] = jnp.concatenate(extra, axis=0).astype(BF)
    for ref in (keep_ref, send_ref):
        ref[count:, half:] = jnp.zeros((16, units), F32)
    for one in copies:
        one.wait()
    p = jnp.dot(z_ref[...], w_ref[...], preferred_element_type=F32)
    low = c_ref[0] == 0
    keep_ref[:, :half] = jnp.where(low, p[:, :half], p[:, half:])
    send_ref[:, :half] = jnp.where(low, p[:, half:], p[:, :half])
    shift = jnp.sum(extra_ref[...].astype(F32), axis=0, keepdims=True)
    shift_ref[...] = jnp.where(low, shift[:, :half], shift[:, half:])


def first_layer(rows, gain, bias, w_all, c_ref, cols):
    n, feats = rows[0].shape
    count = 4 * n
    units = w_all[0].shape[1]
    shape = (count + 16, 3 * units)
    return pl.pallas_call(
        first_kernel,
        out_shape=[jax.ShapeDtypeStruct(shape, F32)] * 2
        + [jax.ShapeDtypeStruct((4 * units, cols), BF), jax.ShapeDtypeStruct((1, 2 * units), F32)],
        in_specs=[SMEM] + [VMEM] * 6 + [ANY] * 4,
        out_specs=[VMEM] * 4,
        scratch_shapes=[
            pltpu.VMEM((count + 16, feats), BF),
            pltpu.VMEM((feats, 4 * units), BF),
            pltpu.VMEM((16, 4 * units), BF),
            pltpu.SemaphoreType.DMA((8 + 4 * (cols // units),)),
        ],
        compiler_params=pltpu.CompilerParams(vmem_limit_bytes=32 << 20),
        cost_estimate=pl.CostEstimate(
            flops=2 * count * feats * 4 * units, bytes_accessed=4 << 20, transcendentals=0
        ),
        name="first_layer",
    )(c_ref, *rows, gain.reshape(1, -1), bias.reshape(1, -1), *w_all)


def pieces(v):
    out = []
    for _ in range(3):
        part = v.astype(BF).astype(F32)
        out.append(part)
        v = v - part
    return out


def pair_kernel(keep_ref, near_ref, out_ref):
    n = out_ref.shape[1] - 16
    count = 4 * n
    wide = out_ref.shape[2]
    half = wide * 2 // 3
    keep, near = keep_ref[:count, :half], near_ref[:count, :half]
    stats_a, stats_b = keep_ref[:count, half:], near_ref[:count, half:]
    mean_a, spread_a = stats_a[:, 0:1], stats_a[:, 1:2]
    mean_b, spread_b = stats_b[:, 0:1], stats_b[:, 1:2]
    tail_a, tail_b = keep_ref[count:, :half], near_ref[count:, :half]
    gain_a = jnp.sum(tail_a[0:3], axis=0, keepdims=True)
    gain_b = jnp.sum(tail_b[0:3], axis=0, keepdims=True)
    shift = jnp.sum(tail_a[3:6] + tail_b[3:6], axis=0, keepdims=True)
    apart = 0.5 * (mean_a - mean_b)
    mean = 0.5 * (mean_a + mean_b)
    spread = 0.5 * (spread_a + spread_b) + apart * apart
    summed = (keep + near + apart * (gain_a - gain_b)).astype(BF)
    columns = pieces(mean) + pieces(spread)
    lane = lax.broadcasted_iota(jnp.int32, (count, wide - half), 1)
    stats = jnp.zeros((count, wide - half), F32)
    for k, column in enumerate(columns):
        stats = jnp.where(lane == k, column, stats)
    stats = stats.astype(BF)
    lower = jnp.concatenate(
        pieces(gain_a + gain_b) + pieces(shift) + [jnp.zeros((10, half), F32)], axis=0
    )
    lower = jnp.concatenate([lower, jnp.zeros((16, wide - half), F32)], axis=1).astype(BF)
    for k in range(4):
        out_ref[k, :n, :half] = summed[k * n : (k + 1) * n]
        out_ref[k, :n, half:] = stats[k * n : (k + 1) * n]
        out_ref[k, n:, :] = lower


def pair_sum(keep, near):
    rows, wide = keep.shape
    n = (rows - 16) // 4
    return pl.pallas_call(
        pair_kernel,
        out_shape=jax.ShapeDtypeStruct((4, n + 16, wide), BF),
        in_specs=[VMEM, VMEM],
        out_specs=VMEM,
        compiler_params=pltpu.CompilerParams(vmem_limit_bytes=16 << 20),
        cost_estimate=pl.CostEstimate(
            flops=10 * rows * wide, bytes_accessed=1 << 20, transcendentals=0
        ),
        name="pair_sum",
    )(keep, near)


def second_kernel(c_ref, at_ref, own_ref, other_ref, w_ref, kept, s1, s2, s3, sum_ref):
    n = kept.shape[0]
    half = own_ref.shape[1]
    low = c_ref[0] == 0
    own, other = own_ref[...].astype(F32), other_ref[...].astype(F32)
    first = jnp.where(low, own, other).astype(BF)
    last = jnp.where(low, other, own).astype(BF)
    sum_ref[...] = jnp.dot(
        first, w_ref[:half, :], preferred_element_type=F32
    ) + jnp.dot(last, w_ref[half:, :], preferred_element_type=F32)
    for k, ref in enumerate((kept, s1, s2, s3)):
        ref[...] = sum_ref[pl.ds(pl.multiple_of(at_ref[k], n), n), :].astype(ref.dtype)


def second_layer(own, other, w_out, c_ref, at):
    count = own.shape[0]
    cols = w_out.shape[1]
    out = (count // 4, cols)
    return pl.pallas_call(
        second_kernel,
        out_shape=[jax.ShapeDtypeStruct(out, F32)] + [jax.ShapeDtypeStruct(out, BF)] * 3,
        in_specs=[SMEM, SMEM] + [VMEM] * 3,
        out_specs=[VMEM] * 4,
        scratch_shapes=[pltpu.VMEM((count, cols), F32)],
        compiler_params=pltpu.CompilerParams(vmem_limit_bytes=16 << 20),
        cost_estimate=pl.CostEstimate(
            flops=4 * count * own.shape[1] * cols, bytes_accessed=1 << 20, transcendentals=0
        ),
        name="second_layer",
    )(c_ref, at, own, other, w_out)


def local(
    patches,
    norm_gain,
    norm_bias,
    proj_in,
    proj_in_bias,
    proj_out,
    proj_out_bias,
    text_rows,
    out_grads,
    gate_weight,
    up_weight,
    down_weight,
    image_counts,
    image_sequence,
    image_offsets,
):
    g, zl, c, zh, x = (lax.axis_index(a) for a in ("g", "zl", "c", "zh", "x"))
    units = proj_in.shape[1]
    width = gate_weight.shape[1]
    cols = text_rows.shape[1]

    patch_other = swap(patches, "zh")
    packed = jnp.concatenate(
        [proj_in]
        + [proj_out[:, k * units : (k + 1) * units] for k in range(cols // units)]
        + [jnp.pad(three_parts(proj_in_bias), ((0, 13), (0, 0)))],
        axis=0,
    )
    w_all = line_of(packed, "g")
    pair = in_order(patches, patch_other, zh)
    rows = line_of(pair, "x")
    own = patches.shape[0]
    count = 8 * own

    side = jnp.concatenate([text_rows, out_grads], axis=1)
    side_other = swap(side, "zh")
    side_pair = in_order(side, side_other, zh)
    side_all = copy_for_each(side_pair, "x").reshape(count, 2 * cols)
    text, cotangent = side_all[:, :cols], side_all[:, cols:]

    half = 2 * units
    c_ref = c.reshape(1).astype(jnp.int32)
    keep, send, w_out, bias = first_layer(rows, norm_gain, norm_bias, w_all, c_ref, cols)
    near = swap(send, "c")
    turns = jnp.arange(4, dtype=jnp.int32)
    n = 2 * own
    parts = lax.all_to_all(pair_sum(keep, near), "zl", 0, 0, tiled=True).astype(F32)
    means = jnp.sum(parts[:, :n, half : half + 3], axis=2, keepdims=True)
    spreads = jnp.sum(parts[:, :n, half + 3 : half + 6], axis=2, keepdims=True)
    gains = jnp.sum(parts[:, n : n + 3, :half], axis=1, keepdims=True)
    shift = jnp.sum(parts[:, n + 3 : n + 6, :half], axis=(0, 1))
    mean = jnp.mean(means, axis=0, keepdims=True)
    spread = jnp.mean(spreads + (means - mean) * (means - mean), axis=0)
    total = jnp.sum(parts[:, :n, :half] + (means - mean) * gains, axis=0)
    total = total * lax.rsqrt(spread + 1e-05) + (shift + bias[0])
    activated = jax.nn.gelu(total, approximate=False).astype(BF)
    act_own = jnp.concatenate(line_of(activated, "zl"), axis=0)
    act_other = swap(act_own, "c")

    part, *sent = second_layer(act_own, act_other, w_out, c_ref, (-turns - zl) % 4 * n)
    for k, v in enumerate(sent):
        part = part + from_next(v, "x", k + 1).astype(F32)
    part = part + swap(part.astype(BF), "zh").astype(F32)
    pair_projected = (part + proj_out_bias).astype(BF)
    projected = jnp.where(zh == 0, pair_projected[:own], pair_projected[own:])
    line_rows = jnp.concatenate(line_of(pair_projected, "x"), axis=0)
    far_rows = [from_next(line_rows, "g", k) for k in (1, 2, 3)]

    q = jnp.arange(count, dtype=jnp.int32)
    block = ((zl + (q // own) % 4) % 4) * 2 + (c + q // (4 * own)) % 2
    at = block * own + q % own
    source, covered = seq_sources(image_counts, image_sequence, image_offsets, g * count + at)

    def gathered_place(r):
        return (r // own) % 4 * (2 * own) + (r // (4 * own)) % 2 * own + r % own

    place = gathered_place(at)

    def x_turned(p):
        return (p - x * (2 * own)) % count

    column = jnp.where(
        covered,
        (source // count - g) % 4 * count + x_turned(gathered_place(source % count)),
        4 * count + place,
    )
    column = lax.optimization_barrier(column)
    choose = column[:, None]
    near_choice = jnp.concatenate([choose == q[None, :], choose == q[None, :] + 4 * count], axis=1)
    far_choice = choose == count + jnp.arange(3 * count)[None, :]
    near_inputs = mm(near_choice.astype(BF), jnp.concatenate([line_rows, text], axis=0))
    far_inputs = mm(far_choice.astype(BF), jnp.concatenate(far_rows, axis=0))
    inputs = (near_inputs + far_inputs).astype(BF)
    z_block = q // own % 4 * 2 + (c + q // (4 * own)) % 2
    reorder = (gathered_place(z_block * own + q % own)[:, None] == q[None, :]).astype(BF)
    back_rows = pick(reorder, cotangent)

    given = mm_t(back_rows[4 * own :], down_weight)
    hidden = mm_t(back_rows[: 4 * own], down_weight)
    there = swap(given, "c")
    near = (hidden + there).astype(BF).reshape(4, own, width)
    hidden_grad = jnp.sum(lax.all_to_all(near, "zl", 0, 0, tiled=True).astype(F32), axis=0)
    whole = jnp.concatenate([mm(inputs, gate_weight), mm(inputs, up_weight)], axis=1)
    total = row_share(whole[: 4 * own], whole[4 * own :], own)
    gate_grad, up_grad = unit_grads(total[:, :width], total[:, width:], hidden_grad)

    grads = jnp.concatenate([gate_grad, up_grad], axis=1)
    line = jnp.concatenate([grads] + [from_next(grads, "zl", k) for k in (1, 2, 3)], axis=0)
    other = swap(line, "c")
    halves = [
        mm_t(h[:, :width], gate_weight) + mm_t(h[:, width:], up_weight) for h in (line, other)
    ]
    turned = jnp.concatenate(halves, axis=0).astype(BF)

    def image_rows(k):
        base = (g - k) % 4 * count
        row = base + (x - q // (2 * own)) % 4 * own + q // own % 2 * (4 * own) + q % own
        target, valid = image_targets(image_counts, image_sequence, image_offsets, row)
        held = valid & (target // count == g)
        return (held[:, None] & ((target % count)[:, None] == at[None, :])).astype(BF)

    back = []
    for k in (2, 1, 3):
        given = pick(image_rows(k), turned)
        back.append(from_next(given, "g", k))
    restore = (q[:, None] == ((x - place // n) % 4 * n + place % n)[None, :]).astype(BF)
    ordered = pick(restore, turned)
    image = mm(image_rows(0), turned) + sum(b.astype(F32) for b in back)
    image = image.astype(BF)
    both = [
        jnp.concatenate([v[k * n : (k + 1) * n] for v in (ordered, image)], axis=0)
        for k in range(4)
    ]
    part = both[0].astype(F32)
    for k in (2, 1, 3):
        part = part + from_next(both[k], "x", k).astype(F32)
    part = part.reshape(2, 2, own, cols)
    keep = jnp.where(zh == 0, part[:, 0], part[:, 1])
    give = jnp.where(zh == 0, part[:, 1], part[:, 0]).astype(BF)
    final = (keep + swap(give, "zh").astype(F32)).astype(BF)
    sequence_grads, row_grads = final[0], final[1]
    return (projected, sequence_grads, row_grads)


def solution(mesh):
    finer = Mesh(mesh.devices.reshape(4, 4, 2, 2, 4), ("g", "zl", "c", "zh", "x"))
    in_specs = (
        P(ROWS, DP),
        P(DP),
        P(DP),
        P(DP, ROWS),
        P(ROWS),
        P(ROWS, DP),
        P(DP),
        P(ROWS, DP),
        P(ROWS, DP),
        P(DP, MP),
        P(DP, MP),
        P(MP, DP),
        P(),
        P(),
        P(),
    )
    out_specs = (P(ROWS, DP), P(ROWS, DP), P(ROWS, DP))
    return jax.shard_map(local, mesh=finer, in_specs=in_specs, out_specs=out_specs, check_vma=False)
```

```python
import jax
import jax.numpy as jnp
from jax import lax
from jax.experimental import pallas as pl
from jax.experimental.pallas import tpu as pltpu
from jax.sharding import Mesh
from jax.sharding import PartitionSpec as P


TOK_DEV = 128
ROWS = ("g", "zh", "x")
DP = ("zl", "c")
MP = ("zh", "x")
BF = jnp.bfloat16
F32 = jnp.float32


def from_next(value, axis, k):
    n = lax.axis_size(axis)
    return lax.ppermute(value, axis, [((i + k) % n, i) for i in range(n)])


def swap(value, axis):
    return lax.ppermute(value, axis, [(0, 1), (1, 0)])


def copy_for_each(shard, axis):
    count = lax.axis_size(axis)
    return lax.all_to_all(
        jnp.broadcast_to(shard[None], (count, *shard.shape)), axis, 0, 0, tiled=True
    )


def in_order(own, other, index, dim=0):
    return jnp.where(
        index == 0,
        jnp.concatenate([own, other], axis=dim),
        jnp.concatenate([other, own], axis=dim),
    )


def line_of(value, axis):
    return [value] + [from_next(value, axis, k) for k in (1, 2, 3)]


def mm(a, b):
    return jnp.dot(a, b, preferred_element_type=F32)


def mm_t(a, b):
    return lax.dot_general(a, b, (((1,), (1,)), ((), ())), preferred_element_type=F32)


def pick(onehot, rows):
    return mm(onehot, rows).astype(BF)


def three_parts(v):
    hi = lax.reduce_precision(v, 8, 7)
    mid = lax.reduce_precision(v - hi, 8, 7)
    low = v - hi - mid
    return jnp.stack([hi, mid, low]).astype(BF)


def seq_sources(counts, sequence, offsets, rows):
    starts = jnp.cumsum(counts) - counts
    seq = rows // TOK_DEV
    pos = rows % TOK_DEV
    hit = (
        (sequence[None, :] == seq[:, None])
        & (offsets[None, :] <= pos[:, None])
        & (pos[:, None] < (offsets + counts)[None, :])
    )
    covered = jnp.any(hit, axis=1)
    source = lax.optimization_barrier(
        jnp.sum(jnp.where(hit, starts[None, :] + pos[:, None] - offsets[None, :], 0), axis=1)
    )
    return (source, covered)


def image_targets(counts, sequence, offsets, rows):
    starts = jnp.cumsum(counts) - counts
    hit = (starts[None, :] <= rows[:, None]) & (rows[:, None] < (starts + counts)[None, :])
    target = jnp.sum(
        jnp.where(
            hit, sequence[None, :] * TOK_DEV + offsets[None, :] + rows[:, None] - starts[None, :], 0
        ),
        axis=1,
    )
    return (target, jnp.any(hit, axis=1))


def unit_grads(gate, up, hidden_grad):
    sig = jax.nn.sigmoid(gate)
    gate_grad = (hidden_grad * up * sig * (1.0 + gate * (1.0 - sig))).astype(BF)
    up_grad = (hidden_grad * gate * sig).astype(BF)
    return (gate_grad, up_grad)


def row_share(kept, given, own):
    there = swap(given, "c")
    near = kept + there
    sent = near[own:].astype(BF)
    total = near[:own]
    for k in (1, 2, 3):
        total = total + from_next(sent[own * (3 - k) : own * (4 - k)], "zl", k).astype(F32)
    return total


VMEM = pl.BlockSpec(memory_space=pltpu.VMEM)
SMEM = pl.BlockSpec(memory_space=pltpu.SMEM)
ANY = pl.BlockSpec(memory_space=pl.ANY)


def first_kernel(
    c_ref, x0, x1, x2, x3, gain_ref, bias_ref, w0, w1, w2, w3, keep_ref, send_ref, z_ref, w_ref, sems
):
    n, feats = x0.shape
    count = 4 * n
    units = w0.shape[1]
    half = 2 * units
    copies = [
        pltpu.make_async_copy(w, w_ref.at[:, pl.ds(k * units, units)], sems.at[k])
        for k, w in enumerate((w0, w1, w2, w3))
    ]
    for copy in copies:
        copy.start()
    gain = gain_ref[...]
    step = n // 4
    lane = lax.broadcasted_iota(jnp.int32, (step, units), 1)
    for k, x_ref in enumerate((x0, x1, x2, x3)):

        @pl.loop(0, 4)
        def _(i):
            x = x_ref[pl.ds(pl.multiple_of(i * step, step), step), :].astype(F32)
            mean = jnp.sum(x, axis=1, keepdims=True) * (1.0 / feats)
            centred = x - mean
            spread = jnp.sum(centred * centred, axis=1, keepdims=True) * (1.0 / feats)
            rows = pl.ds(pl.multiple_of(k * n + i * step, step), step)
            z_ref[rows, :] = (centred * gain).astype(BF)
            stats = jnp.where(lane == 0, mean, jnp.where(lane == 1, spread, 0.0))
            for ref in (keep_ref, send_ref):
                ref[rows, half:] = stats

    extra = []
    for v in (gain, bias_ref[...]):
        for _ in range(3):
            part = v.astype(BF).astype(F32)
            extra.append(part)
            v = v - part
    extra.append(jnp.zeros((10, feats), F32))
    z_ref[count:, :] = jnp.concatenate(extra, axis=0).astype(BF)
    for ref in (keep_ref, send_ref):
        ref[count:, half:] = jnp.zeros((16, units), F32)
    for copy in copies:
        copy.wait()
    p = jnp.dot(z_ref[...], w_ref[...], preferred_element_type=F32)
    low = c_ref[0] == 0
    keep_ref[:, :half] = jnp.where(low, p[:, :half], p[:, half:])
    send_ref[:, :half] = jnp.where(low, p[:, half:], p[:, :half])


def first_layer(rows, gain, bias, w_in, c_ref):
    n, feats = rows[0].shape
    count = 4 * n
    units = w_in[0].shape[1]
    shape = (count + 16, 3 * units)
    return pl.pallas_call(
        first_kernel,
        out_shape=[jax.ShapeDtypeStruct(shape, F32)] * 2,
        in_specs=[SMEM] + [VMEM] * 6 + [ANY] * 4,
        out_specs=[VMEM, VMEM],
        scratch_shapes=[
            pltpu.VMEM((count + 16, feats), BF),
            pltpu.VMEM((feats, 4 * units), BF),
            pltpu.SemaphoreType.DMA((4,)),
        ],
        compiler_params=pltpu.CompilerParams(vmem_limit_bytes=32 << 20),
        cost_estimate=pl.CostEstimate(
            flops=2 * count * feats * 4 * units, bytes_accessed=4 << 20, transcendentals=0
        ),
        name="first_layer",
    )(c_ref, *rows, gain.reshape(1, -1), bias.reshape(1, -1), *w_in)


def pieces(v):
    out = []
    for _ in range(3):
        part = v.astype(BF).astype(F32)
        out.append(part)
        v = v - part
    return out


def pair_kernel(keep_ref, near_ref, out_ref):
    n = out_ref.shape[1] - 16
    count = 4 * n
    wide = out_ref.shape[2]
    half = wide * 2 // 3
    keep, near = keep_ref[:count, :half], near_ref[:count, :half]
    stats_a, stats_b = keep_ref[:count, half:], near_ref[:count, half:]
    mean_a, spread_a = stats_a[:, 0:1], stats_a[:, 1:2]
    mean_b, spread_b = stats_b[:, 0:1], stats_b[:, 1:2]
    tail_a, tail_b = keep_ref[count:, :half], near_ref[count:, :half]
    gain_a = jnp.sum(tail_a[0:3], axis=0, keepdims=True)
    gain_b = jnp.sum(tail_b[0:3], axis=0, keepdims=True)
    shift = jnp.sum(tail_a[3:6] + tail_b[3:6], axis=0, keepdims=True)
    apart = 0.5 * (mean_a - mean_b)
    mean = 0.5 * (mean_a + mean_b)
    spread = 0.5 * (spread_a + spread_b) + apart * apart
    summed = (keep + near + apart * (gain_a - gain_b)).astype(BF)
    columns = pieces(mean) + pieces(spread)
    lane = lax.broadcasted_iota(jnp.int32, (count, wide - half), 1)
    stats = jnp.zeros((count, wide - half), F32)
    for k, column in enumerate(columns):
        stats = jnp.where(lane == k, column, stats)
    stats = stats.astype(BF)
    lower = jnp.concatenate(
        pieces(gain_a + gain_b) + pieces(shift) + [jnp.zeros((10, half), F32)], axis=0
    )
    lower = jnp.concatenate([lower, jnp.zeros((16, wide - half), F32)], axis=1).astype(BF)
    for k in range(4):
        out_ref[k, :n, :half] = summed[k * n : (k + 1) * n]
        out_ref[k, :n, half:] = stats[k * n : (k + 1) * n]
        out_ref[k, n:, :] = lower


def pair_sum(keep, near):
    rows, wide = keep.shape
    n = (rows - 16) // 4
    return pl.pallas_call(
        pair_kernel,
        out_shape=jax.ShapeDtypeStruct((4, n + 16, wide), BF),
        in_specs=[VMEM, VMEM],
        out_specs=VMEM,
        compiler_params=pltpu.CompilerParams(vmem_limit_bytes=16 << 20),
        cost_estimate=pl.CostEstimate(
            flops=10 * rows * wide, bytes_accessed=1 << 20, transcendentals=0
        ),
        name="pair_sum",
    )(keep, near)


def second_kernel(c_ref, at_ref, own_ref, other_ref, w_ref, kept, s1, s2, s3, sum_ref):
    n = kept.shape[0]
    units = w_ref.shape[1] - 16
    low = c_ref[0] == 0
    total = jnp.zeros(sum_ref.shape, F32)
    for j in range(4):
        at = slice((j % 2) * units, (j % 2 + 1) * units)
        a, b = (own_ref, other_ref) if j < 2 else (other_ref, own_ref)
        act = jnp.where(low, a[:, at].astype(F32), b[:, at].astype(F32)).astype(BF)
        total += jnp.dot(act, w_ref[at_ref[4 + j], :units, :], preferred_element_type=F32)
    sum_ref[...] = total
    for k, ref in enumerate((kept, s1, s2, s3)):
        ref[...] = sum_ref[pl.ds(pl.multiple_of(at_ref[k], n), n), :].astype(ref.dtype)


def second_layer(own, other, w_out, c_ref, at):
    count = own.shape[0]
    cols = w_out.shape[2]
    out = (count // 4, cols)
    return pl.pallas_call(
        second_kernel,
        out_shape=[jax.ShapeDtypeStruct(out, F32)] + [jax.ShapeDtypeStruct(out, BF)] * 3,
        in_specs=[SMEM, SMEM] + [VMEM] * 3,
        out_specs=[VMEM] * 4,
        scratch_shapes=[pltpu.VMEM((count, cols), F32)],
        compiler_params=pltpu.CompilerParams(vmem_limit_bytes=16 << 20),
        cost_estimate=pl.CostEstimate(
            flops=4 * count * own.shape[1] * cols, bytes_accessed=1 << 20, transcendentals=0
        ),
        name="second_layer",
    )(c_ref, at, own, other, w_out)


def local(
    patches,
    norm_gain,
    norm_bias,
    proj_in,
    proj_in_bias,
    proj_out,
    proj_out_bias,
    text_rows,
    out_grads,
    gate_weight,
    up_weight,
    down_weight,
    image_counts,
    image_sequence,
    image_offsets,
):
    g, zl, c, zh, x = (lax.axis_index(a) for a in ("g", "zl", "c", "zh", "x"))
    units = proj_in.shape[1]
    width = gate_weight.shape[1]
    cols = text_rows.shape[1]

    patch_other = swap(patches, "zh")
    w_in = [proj_in] + [from_next(proj_in, "g", k) for k in (1, 2, 3)]
    packed = jnp.concatenate(
        [proj_out, jnp.pad(three_parts(proj_in_bias), ((0, 13), (0, cols - units)))], axis=0
    )
    w_out = copy_for_each(packed, "g")
    pair = in_order(patches, patch_other, zh)
    rows = line_of(pair, "x")
    own = patches.shape[0]
    count = 8 * own

    side = jnp.concatenate([text_rows, out_grads], axis=1)
    side_other = swap(side, "zh")
    side_pair = in_order(side, side_other, zh)
    side_all = jnp.concatenate(line_of(side_pair, "x"), axis=0)
    text, cotangent = side_all[:, :cols], side_all[:, cols:]

    half = 2 * units
    c_ref = c.reshape(1).astype(jnp.int32)
    keep, send = first_layer(rows, norm_gain, norm_bias, w_in, c_ref)
    near = swap(send, "c")
    turns = jnp.arange(4, dtype=jnp.int32)
    n = 2 * own
    order = (g + turns) % 4
    bias = jnp.sum(w_out[:, units : units + 3, :units].astype(F32), axis=1)
    bias = jnp.where((order[:, None] == turns[None, :])[:, :, None], bias[None], 0.0)
    bias = lax.optimization_barrier(jnp.sum(bias, axis=1).reshape(-1))
    bias = jnp.where(c == 0, bias[:half], bias[half:])
    parts = lax.all_to_all(pair_sum(keep, near), "zl", 0, 0, tiled=True).astype(F32)
    means = jnp.sum(parts[:, :n, half : half + 3], axis=2, keepdims=True)
    spreads = jnp.sum(parts[:, :n, half + 3 : half + 6], axis=2, keepdims=True)
    gains = jnp.sum(parts[:, n : n + 3, :half], axis=1, keepdims=True)
    shift = jnp.sum(parts[:, n + 3 : n + 6, :half], axis=(0, 1))
    mean = jnp.mean(means, axis=0, keepdims=True)
    spread = jnp.mean(spreads + (means - mean) * (means - mean), axis=0)
    total = jnp.sum(parts[:, :n, :half] + (means - mean) * gains, axis=0)
    total = total * lax.rsqrt(spread + 1e-05) + (shift + bias)
    activated = jax.nn.gelu(total, approximate=False).astype(BF)
    act_own = copy_for_each(activated, "zl").reshape(count, half)
    act_other = swap(act_own, "c")

    part, *sent = second_layer(act_own, act_other, w_out, c_ref, jnp.concatenate([-turns % 4 * n, order]))
    for k, v in enumerate(sent):
        part = part + from_next(v, "x", k + 1).astype(F32)
    part = part + swap(part.astype(BF), "zh").astype(F32)
    pair_projected = (part + proj_out_bias).astype(BF)
    projected = jnp.where(zh == 0, pair_projected[:own], pair_projected[own:])
    line_rows = jnp.concatenate(line_of(pair_projected, "x"), axis=0)
    far_rows = [from_next(line_rows, "g", k) for k in (1, 2, 3)]

    q = jnp.arange(count, dtype=jnp.int32)
    block = ((zl + (q // own) % 4) % 4) * 2 + (c + q // (4 * own)) % 2
    at = block * own + q % own
    source, covered = seq_sources(image_counts, image_sequence, image_offsets, g * count + at)

    def gathered_place(r):
        return (r // own) % 4 * (2 * own) + (r // (4 * own)) % 2 * own + r % own

    place = gathered_place(at)

    def x_turned(p):
        return (p - x * (2 * own)) % count

    text_place = x_turned(place)
    column = jnp.where(
        covered,
        (source // count - g) % 4 * count + x_turned(gathered_place(source % count)),
        4 * count + text_place,
    )
    column = lax.optimization_barrier(column)
    choose = column[:, None]
    near_choice = jnp.concatenate([choose == q[None, :], choose == q[None, :] + 4 * count], axis=1)
    far_choice = choose == count + jnp.arange(3 * count)[None, :]
    near_inputs = mm(near_choice.astype(BF), jnp.concatenate([line_rows, text], axis=0))
    far_inputs = mm(far_choice.astype(BF), jnp.concatenate(far_rows, axis=0))
    inputs = (near_inputs + far_inputs).astype(BF)
    z_block = q // own % 4 * 2 + (c + q // (4 * own)) % 2
    reorder = x_turned(gathered_place(z_block * own + q % own))
    reorder = (reorder[:, None] == q[None, :]).astype(BF)
    back_rows = pick(reorder, cotangent)

    given = mm_t(back_rows[4 * own :], down_weight)
    hidden = mm_t(back_rows[: 4 * own], down_weight)
    there = swap(given, "c")
    near = (hidden + there).astype(BF).reshape(4, own, width)
    hidden_grad = jnp.sum(lax.all_to_all(near, "zl", 0, 0, tiled=True).astype(F32), axis=0)
    whole = jnp.concatenate([mm(inputs, gate_weight), mm(inputs, up_weight)], axis=1)
    total = row_share(whole[: 4 * own], whole[4 * own :], own)
    gate_grad, up_grad = unit_grads(total[:, :width], total[:, width:], hidden_grad)

    grads = jnp.concatenate([gate_grad, up_grad], axis=1)
    line = jnp.concatenate([grads] + [from_next(grads, "zl", k) for k in (1, 2, 3)], axis=0)
    other = swap(line, "c")
    halves = [
        mm_t(h[:, :width], gate_weight) + mm_t(h[:, width:], up_weight) for h in (line, other)
    ]
    turned = jnp.concatenate(halves, axis=0).astype(BF)

    def image_rows(k):
        base = (g - k) % 4 * count
        row = base + (x - q // (2 * own)) % 4 * own + q // own % 2 * (4 * own) + q % own
        target, valid = image_targets(image_counts, image_sequence, image_offsets, row)
        held = valid & (target // count == g)
        return (held[:, None] & ((target % count)[:, None] == at[None, :])).astype(BF)

    back = []
    for k in (2, 1, 3):
        given = pick(image_rows(k), turned)
        back.append(from_next(given, "g", k))
    restore = (q[:, None] == ((x - place // n) % 4 * n + place % n)[None, :]).astype(BF)
    ordered = pick(restore, turned)
    image = mm(image_rows(0), turned) + sum(b.astype(F32) for b in back)
    image = image.astype(BF)
    both = [
        jnp.concatenate([v[k * n : (k + 1) * n] for v in (ordered, image)], axis=0)
        for k in range(4)
    ]
    part = both[0].astype(F32)
    for k in (2, 1, 3):
        part = part + from_next(both[k], "x", k).astype(F32)
    part = part.reshape(2, 2, own, cols)
    keep = jnp.where(zh == 0, part[:, 0], part[:, 1])
    give = jnp.where(zh == 0, part[:, 1], part[:, 0]).astype(BF)
    final = (keep + swap(give, "zh").astype(F32)).astype(BF)
    sequence_grads, row_grads = final[0], final[1]
    return (projected, sequence_grads, row_grads)


def solution(mesh):
    finer = Mesh(mesh.devices.reshape(4, 4, 2, 2, 4), ("g", "zl", "c", "zh", "x"))
    in_specs = (
        P(ROWS, DP),
        P(DP),
        P(DP),
        P(DP, ROWS),
        P(ROWS),
        P(ROWS, DP),
        P(DP),
        P(ROWS, DP),
        P(ROWS, DP),
        P(DP, MP),
        P(DP, MP),
        P(MP, DP),
        P(),
        P(),
        P(),
    )
    out_specs = (P(ROWS, DP), P(ROWS, DP), P(ROWS, DP))
    return jax.shard_map(local, mesh=finer, in_specs=in_specs, out_specs=out_specs, check_vma=False)
```
